32 devices in a mesh: px: 2 (over core), pz: 16 (over z, y, x).
Axes of the slice: x: 2, y: 2, z: 4, core: 2. Of those that a mesh axis runs over, the one named last changes fastest.
Arguments:
- velocity: float32 [3, 256, 32, 256], P(None, 'pz', None, 'px'), may hold values from -8 to 8, as said below
- filter_inverse: float32 [256, 256], replicated, may hold values from 0 to 2, as said below
- filter_block: int32 [256], replicated, may hold values from 0 to 7, never falling along the last dimension, each value on 1 to 128 neighbouring positions
- plane_bin: int32 [256], replicated, may hold values from 0 to 63, never falling along the last dimension, each value on 1 to 16 neighbouring positions
Outputs:
- leonard: float32 [6, 256, 32, 256], P(None, 'pz', None, 'px')
- viscosity: float32 [256, 32, 256], P('pz', None, 'px')
- coefficient: float32 [256], replicated
The draws below stay inside these ranges and needn't reach their ends.
Inputs may be any that keep to these rules, and one draw needn't show every extreme that they name: `velocity`: each component is a rough random field. `filter_inverse`: entries are positive. `filter_block`: never falls along the planes; each of the 8 blocks holds 1 to 128 consecutive planes, one exactly 128. `plane_bin`: never falls along the planes; each of the 64 bins holds 1 to 16 consecutive planes, one exactly 16.
All inputs are finite; a program needn't handle non-finite values.
Results may differ from the reference program's by a relative error of at most 0.0003.
Values sent between devices are 32-bit elements; how exact they have to be, the bound alone decides.
A program may use at most 128 MiB of HBM per device.

```python
import math
import jax
import jax.numpy as jnp
import numpy as np
from jax import lax

NY = 256
NFB = 8
FBMOST = 128
NBIN = 64
BINMOST = 16
NX = 256
NZ = 32


def draw_velocity(key, part):
    noise_key, scale_key = jax.random.split(jax.random.fold_in(key, 11))
    base = jax.random.normal(noise_key, (3, NY, NZ, NX), jnp.float32)
    amplitude = jnp.exp(jax.random.uniform(scale_key, (1, 1, NZ, NX // 8), jnp.float32, -0.7, 0.7))
    amplitude = jnp.repeat(amplitude, 8, axis=3)
    return jnp.clip(base * amplitude, -8.0, 8.0)


def draw_filter_inverse(key, part):
    entry_key = jax.random.fold_in(key, 23)
    rows = jnp.arange(NY, dtype=jnp.float32)
    distance = jnp.abs(rows[:, None] - rows[None, :])
    factors = jax.random.uniform(entry_key, (NY, NY), jnp.float32, 0.5, 1.5)
    return jnp.exp(-distance / 256.0) * factors


def split_up(number_of, total, bound, slope):
    loads = [(1 << 20) // math.isqrt(grade ** slope) + 1 for grade in range(2, number_of + 1)]
    spare, holding = total - bound - (number_of - 1), [1] * (number_of - 1)
    while spare > 0:
        free = [i for i in range(number_of - 1) if holding[i] < bound]
        whole, budget = sum([loads[i] for i in free]), spare
        for i in free:
            extra = min(bound - holding[i], max(1, budget * loads[i] // whole), spare)
            holding[i] = holding[i] + extra
            spare = spare - extra
    return np.array([bound] + holding)


def ragged_sizes(rng, count, total, reach, lean):
    if count == 2:
        one = jax.random.randint(rng, (), max(1, total - reach), min(reach, total - 1) + 1)
        return jnp.stack([one, total - one])
    sizes = jnp.asarray(split_up(count, total, reach, lean), jnp.int32)
    couples = (count - 1) // 2
    donor, sink = sizes[1:1 + 2 * couples:2], sizes[2:2 + 2 * couples:2]
    room = jnp.minimum(donor - 1, reach - sink)
    shifted = jax.random.randint(jax.random.fold_in(rng, 1), (couples,), 0, 1 << 20) % (room + 1)
    sizes = sizes.at[1:1 + 2 * couples:2].set(donor - shifted).at[2:2 + 2 * couples:2].set(sink + shifted)
    return sizes[jax.random.permutation(jax.random.fold_in(rng, 2), count)]


def setup_inputs(seed: int = 0) -> dict:
    keys = jax.random.split(jax.random.key(seed), 5)
    velocity = draw_velocity(jax.random.fold_in(keys[4], 71), 0)
    filter_inverse = draw_filter_inverse(jax.random.fold_in(keys[4], 71), 0)
    filter_block = jnp.searchsorted(jnp.cumsum(ragged_sizes(keys[2], NFB, NY, FBMOST, 1)), jnp.arange(NY), side="right").astype(jnp.int32)
    plane_bin = jnp.searchsorted(jnp.cumsum(ragged_sizes(keys[3], NBIN, NY, BINMOST, 1)), jnp.arange(NY), side="right").astype(jnp.int32)
    return dict(velocity=velocity, filter_inverse=filter_inverse, filter_block=filter_block, plane_bin=plane_bin)


def block_weights(filter_inverse, filter_block):
    same = (filter_block[:, None] == filter_block[None, :]).astype(jnp.float32)
    masked = filter_inverse * same
    return masked / lax.optimization_barrier(jnp.sum(masked, axis=1, keepdims=True))

def quantities(padded):
    centre = padded[:, 1:-1, 1:-1, 1:-1]
    along_y = (padded[:, 2:, 1:-1, 1:-1] - padded[:, :-2, 1:-1, 1:-1]) * 0.5
    along_z = (padded[:, 1:-1, 2:, 1:-1] - padded[:, 1:-1, :-2, 1:-1]) * 0.5
    along_x = (padded[:, 1:-1, 1:-1, 2:] - padded[:, 1:-1, 1:-1, :-2]) * 0.5
    strain = jnp.stack([along_x[0], along_y[1], along_z[2], 0.5 * (along_y[0] + along_x[1]), 0.5 * (along_z[0] + along_x[2]), 0.5 * (along_z[1] + along_y[2])])
    magnitude = jnp.sqrt(2.0 * lax.optimization_barrier(jnp.sum(strain[:3] * strain[:3], axis=0)) + 4.0 * lax.optimization_barrier(jnp.sum(strain[3:] * strain[3:], axis=0)))
    products = jnp.stack([centre[0] * centre[0], centre[1] * centre[1], centre[2] * centre[2], centre[0] * centre[1], centre[0] * centre[2], centre[1] * centre[2]])
    fields = jnp.concatenate([centre, strain, products, magnitude[None] * strain], axis=0)
    along = (fields[..., :-2] + 2.0 * fields[..., 1:-1] + fields[..., 2:]) * 0.25
    boxed = (along[:, :, :-2] + 2.0 * along[:, :, 1:-1] + along[:, :, 2:]) * 0.25
    return (boxed, magnitude[:, 1:-1, 1:-1])

def contract(filtered):
    speed = filtered[0:3]
    strain = filtered[3:9]
    products = filtered[9:15]
    scaled = filtered[15:21]
    leonard = products - jnp.stack([speed[0] * speed[0], speed[1] * speed[1], speed[2] * speed[2], speed[0] * speed[1], speed[0] * speed[2], speed[1] * speed[2]])
    fmag = jnp.sqrt(2.0 * lax.optimization_barrier(jnp.sum(strain[:3] * strain[:3], axis=0)) + 4.0 * lax.optimization_barrier(jnp.sum(strain[3:] * strain[3:], axis=0)))
    model = scaled - 4.0 * fmag[None] * strain
    weights = jnp.array([1.0, 1.0, 1.0, 2.0, 2.0, 2.0], jnp.float32).reshape(6, 1, 1, 1)
    product_lm = lax.optimization_barrier(jnp.sum(weights * leonard * model, axis=0))
    product_mm = lax.optimization_barrier(jnp.sum(weights * model * model, axis=0))
    return (leonard, product_lm, product_mm)

def reference(velocity, filter_inverse, filter_block, plane_bin):
    weights = block_weights(filter_inverse, filter_block)

    def one_plane(plane):
        indices = ((plane + jnp.arange(-2, 3, dtype=jnp.int32)) % NZ).astype(jnp.int32)
        window = jnp.take(velocity, indices, axis=2)
        window = jnp.pad(window, ((0, 0), (1, 1), (0, 0), (0, 0)))
        window = jnp.concatenate([window[..., -2:], window, window[..., :2]], axis=3)
        boxed, magnitude = quantities(window)
        filtered = jnp.einsum('ab,kbzx->kazx', weights, boxed, precision=lax.Precision.HIGHEST)
        leonard, product_lm, product_mm = contract(filtered)
        return (leonard[:, :, 0, :], lax.optimization_barrier(jnp.sum(product_lm, axis=(1, 2))), lax.optimization_barrier(jnp.sum(product_mm, axis=(1, 2))), magnitude[:, 0, :])
    leonard, plane_lm, plane_mm, magnitude = lax.map(one_plane, jnp.arange(NZ, dtype=jnp.int32))
    plane_lm = lax.optimization_barrier(jnp.sum(plane_lm, axis=0))
    plane_mm = lax.optimization_barrier(jnp.sum(plane_mm, axis=0))
    onehot = (plane_bin[:, None] == jnp.arange(NBIN, dtype=jnp.int32)[None, :]).astype(jnp.float32)
    numer = jnp.dot(plane_lm, onehot, precision=lax.Precision.HIGHEST)
    denom = jnp.dot(plane_mm, onehot, precision=lax.Precision.HIGHEST)
    per_bin = numer / jnp.maximum(denom, jnp.float32(NX * NZ))
    coefficient = jnp.dot(onehot, per_bin, precision=lax.Precision.HIGHEST)
    leonard = jnp.transpose(leonard, (1, 2, 0, 3))
    viscosity = coefficient[:, None, None] * jnp.transpose(magnitude, (1, 0, 2))
    return (leonard, viscosity, coefficient)
```

```python
import functools

import jax
import jax.numpy as jnp
from jax import lax
from jax.experimental import pallas as pl
from jax.experimental.pallas import tpu as pltpu
from jax.sharding import PartitionSpec as P

NBIN = 64
MESH = pl.DeviceIdType.MESH
PAIRS = ((0, 0), (1, 1), (2, 2), (0, 1), (0, 2), (1, 2))


def tensor_norm(s):
    diag = s[0] * s[0] + s[1] * s[1] + s[2] * s[2]
    off = s[3] * s[3] + s[4] * s[4] + s[5] * s[5]
    return jnp.sqrt(2.0 * diag + 4.0 * off)


def strain_of(dx, dy, dz):
    return [
        dx[0] * 0.5,
        dy[1] * 0.5,
        dz[2] * 0.5,
        0.25 * (dy[0] + dx[1]),
        0.25 * (dz[0] + dx[2]),
        0.25 * (dz[1] + dy[2]),
    ]


def fill_from_blocks(dims, ext, own, right, left):
    n, win, lp, nx = dims
    lane = lax.broadcasted_iota(jnp.int32, (lp, nx), 1)
    from_right = lane < nx // 2

    @pl.loop(0, n)
    def _(p):
        rows = pl.ds(pl.multiple_of(8 + p * lp, 8), lp)
        for c in range(3):
            for z in range(win):
                ext[c, z, rows, 0:nx] = own[p, c, z]
                ext[c, z, rows, nx : 2 * nx] = jnp.where(from_right, right[p, c, z], left[p, c, z])


def column_kernel(dims, fill, sources, *refs):
    n, win, lp, nx = dims
    blocks, refs = refs[:sources], refs[sources:]
    weights, onehot, back, ext, bhi, blo, filt, lms, mms, whi, wlo = refs
    zs = win - 4
    ny = n * lp
    lanes = 2 * nx
    heavy = weights[...].astype(jnp.bfloat16)
    whi[...] = heavy
    wlo[...] = (weights[...] - heavy.astype(jnp.float32)).astype(jnp.bfloat16)

    zero = jnp.zeros((8, lanes), jnp.float32)
    for c in range(3):
        for z in range(win):
            ext[c, z, 0:8, :] = zero
            ext[c, z, ny + 8 : ny + 16, :] = zero
    fill(dims, ext, *blocks)

    @pl.loop(0, n)
    def _(p):
        base = pl.multiple_of(p * lp, 8)
        u = [[ext[c, z, pl.ds(base + 8, lp), :] for z in range(win)] for c in range(3)]
        boxes = [[None] * 21 for _ in range(zs)]
        for z in range(1, win - 1):
            v = [u[c][z] for c in range(3)]
            dx, dy, dz = [], [], []
            for c in range(3):
                dx.append(pltpu.roll(v[c], lanes - 1, 1) - pltpu.roll(v[c], 1, 1))
                tall = ext[c, z, pl.ds(base, lp + 16), :]
                dy.append(tall[9 : 9 + lp] - tall[7 : 7 + lp])
                dz.append(u[c][z + 1] - u[c][z - 1])
            s = strain_of(dx, dy, dz)
            mag = tensor_norm(s)
            fields = v + s + [v[i] * v[j] for i, j in PAIRS] + [mag * t for t in s]
            for o in range(zs):
                step = z - (o + 2)
                if -1 <= step <= 1:
                    for k in range(21):
                        term = fields[k] if step else 2.0 * fields[k]
                        boxes[o][k] = term if boxes[o][k] is None else boxes[o][k] + term
        for o in range(zs):
            for k in range(21):
                f = boxes[o][k]
                box = (pltpu.roll(f, 1, 1) + pltpu.roll(f, lanes - 1, 1) + 2.0 * f)[:, :nx] * 0.0625
                high = box.astype(jnp.bfloat16)
                cols = slice(o * nx, (o + 1) * nx)
                bhi[k, pl.ds(base, lp), cols] = high
                blo[k, pl.ds(base, lp), cols] = (box - high.astype(jnp.float32)).astype(jnp.bfloat16)

    @pl.loop(0, 21)
    def _(k):
        dot = functools.partial(jnp.dot, preferred_element_type=jnp.float32)
        filt[k] = dot(whi[...], bhi[k]) + (dot(whi[...], blo[k]) + dot(wlo[...], bhi[k]))

    @pl.loop(0, n)
    def _(p):
        base = pl.multiple_of(p * lp, 8)
        lm_total = jnp.zeros((lp, nx), jnp.float32)
        mm_total = jnp.zeros((lp, nx), jnp.float32)
        for o in range(zs):
            g = [filt[k, pl.ds(base, lp), o * nx : (o + 1) * nx] for k in range(21)]
            fmag = 4.0 * tensor_norm(g[3:9])
            for q, (i, j) in enumerate(PAIRS):
                leonard = g[9 + q] - g[i] * g[j]
                model = g[15 + q] - fmag * g[3 + q]
                weighted = model if q < 3 else 2.0 * model
                lm_total += leonard * weighted
                mm_total += model * weighted
                back[p, (q * zs + o) * lp : (q * zs + o + 1) * lp, :] = leonard
        lms[pl.ds(base, lp), :] = lm_total
        mms[pl.ds(base, lp), :] = mm_total

    ones = jnp.ones((8, nx), jnp.float32)
    exact = functools.partial(
        lax.dot_general, preferred_element_type=jnp.float32, precision=lax.Precision.HIGHEST
    )
    totals = []
    for part in (lms, mms):
        planes = exact(ones, part[...], (((1,), (1,)), ((), ())))
        totals.append(exact(planes, onehot[...], (((1,), (0,)), ((), ()))))
    row = lax.broadcasted_iota(jnp.int32, (8, onehot.shape[1]), 0)
    tile = jnp.where(row < 4, totals[0], totals[1])
    for p in range(n):
        back[p, 6 * zs * lp :, :] = tile


def greet_all(m, n):
    me = lax.axis_index("px") * n + lax.axis_index("pz")
    barrier = pltpu.get_barrier_semaphore()

    @pl.loop(1, m * n)
    def _(step):
        peer = lax.rem(me + step, m * n)
        pl.semaphore_signal(barrier, inc=1, device_id=(peer // n, lax.rem(peer, n)), device_id_type=MESH)

    pl.semaphore_wait(barrier, m * n - 1)


def magnitude_kernel(centre, right, left, below, above, out):
    _, lp, nz, nx = centre.shape
    lane = lax.broadcasted_iota(jnp.int32, (nz, nx), 1)
    for y in range(lp):
        v = [centre[c, y] for c in range(3)]
        dx, dy, dz = [], [], []
        for c in range(3):
            ahead = jnp.where(lane == nx - 1, pltpu.roll(right[c, y], nx - 1, 1), pltpu.roll(v[c], nx - 1, 1))
            behind = jnp.where(lane == 0, pltpu.roll(left[c, y], 1, 1), pltpu.roll(v[c], 1, 1))
            dx.append(ahead - behind)
            dz.append(pltpu.roll(v[c], nz - 1, 0) - pltpu.roll(v[c], 1, 0))
            up = centre[c, y + 1] if y + 1 < lp else above[c, 0]
            down = centre[c, y - 1] if y else below[c, 0]
            dy.append(up - down)
        out[y] = tensor_norm(strain_of(dx, dy, dz))


def swap_bit(first, second, bit):
    nx = first.shape[-1]
    low = (lax.broadcasted_iota(jnp.int32, first.shape, 1) & bit) == 0
    return (
        jnp.where(low, first, pltpu.roll(second, bit, 1)),
        jnp.where(low, pltpu.roll(first, nx - bit, 1), second),
    )


def pack_kernel(dims, velocity, packed):
    lp, nz, nx = dims
    groups = nx // nz
    steps = lp // groups

    @pl.loop(0, 3)
    def _(c):
        for q in range(steps):
            rows = jnp.concatenate([velocity[c, g * steps + q] for g in range(groups)], axis=0)
            packed[c, pl.ds(q, nx, stride=steps), :] = rows.T


def spread_kernel(dims, packed, held, main_out, left_out, right_out, pass_out, main_in, edge_in, pass_in):
    n, h, pairs = dims
    a, s = lax.axis_index("px"), lax.axis_index("pz")
    greet_all(2, n)

    def send(source, dst, core, chip, out_sem, in_sem):
        itself = (core == a) & (chip == s)
        copy = pltpu.make_async_remote_copy(
            source, dst, out_sem, in_sem, device_id=(core, chip), device_id_type=MESH
        )
        return itself, copy, pltpu.make_async_copy(source, dst, in_sem)

    def sends(i):
        chip = h * a + i
        whole = 2 * pairs
        for core in range(2):
            source = packed.at[:, pl.ds(whole * i + pairs * core, pairs)]
            yield send(source, held.at[s, :, 1 : pairs + 1], core, chip, main_out.at[i, core], main_in.at[s])
        source = packed.at[:, pl.ds(whole * i + whole - 1, 1)]
        yield send(source, held.at[s, :, 0:1], 0, lax.rem(chip + 1, n), left_out.at[i], edge_in.at[s])
        source = packed.at[:, pl.ds(whole * i, 1)]
        yield send(source, held.at[s, :, pairs + 1 : pairs + 2], 1, lax.rem(chip + n - 1, n), right_out.at[i], edge_in.at[s])

    @pl.loop(0, h)
    def _(r):
        for itself, copy, here in sends(lax.rem(s + r, h)):
            pl.when(itself)(here.start)
            pl.when(jnp.logical_not(itself))(copy.start)

    def forward(p):
        source = held.at[p, :, pl.ds(pairs - (pairs - 1) * a, 1)]
        return pltpu.make_async_remote_copy(
            source, held.at[p, :, pl.ds((pairs + 1) * a, 1)], pass_out.at[p], pass_in.at[p],
            device_id=(1 - a, s), device_id_type=MESH,
        )

    @pl.loop(0, n)
    def _(i):
        p = lax.rem(s + n - i, n)
        pltpu.make_async_copy(packed.at[:, 0:pairs], held.at[p, :, 1 : pairs + 1], main_in.at[p]).wait()
        forward(p).start()

    @pl.loop(0, n)
    def _(p):
        forward(p).wait()
        pltpu.make_async_copy(packed.at[:, 0:1], held.at[p, :, 0:1], edge_in.at[p]).wait()

    @pl.loop(0, h)
    def _(i):
        for itself, copy, here in sends(i):
            pl.when(jnp.logical_not(itself))(copy.wait_send)


def plane_order(shape, lp, nx, dim):
    at = lax.broadcasted_iota(jnp.int32, shape, dim)
    return (at % nx) // 8 * lp + at // nx * 8 + at % 8


def column_weights(dims, inverse, block, bins, whi, wlo, onehot):
    ny, lp, nx = dims
    label = jnp.broadcast_to(block[...].astype(jnp.float32), (ny, ny))
    masked = jnp.where(label == label.T, inverse[...], 0.0)
    weights = masked / jnp.sum(masked, axis=1, keepdims=True) * 0.0625
    order = plane_order((ny, ny), lp, nx, 0) == lax.broadcasted_iota(jnp.int32, (ny, ny), 1)
    order = order.astype(jnp.float32).astype(jnp.bfloat16)
    across = functools.partial(
        lax.dot_general, dimension_numbers=(((1,), (1,)), ((), ())), preferred_element_type=jnp.float32
    )

    def placed(part):
        turned = across(order, part).astype(jnp.bfloat16)
        return across(turned, order).astype(jnp.bfloat16)

    heavy = weights.astype(jnp.bfloat16)
    whi[...] = placed(heavy)
    wlo[...] = placed((weights - heavy.astype(jnp.float32)).astype(jnp.bfloat16))
    label = jnp.broadcast_to(bins[...], (nx, ny))
    hot = (label == lax.broadcasted_iota(jnp.int32, (nx, ny), 0)).astype(jnp.float32)
    onehot[...] = across(hot.astype(jnp.bfloat16), order)


def strip_kernel(dims, held, inverse, block, bins, back, u, fields, filt, stress, whi, wlo, onehot, sums):
    n, pairs, lp, nz, nx = dims
    ny, groups = n * lp, nx // nz
    halves = lp // 8
    across = 2 * pairs
    tiles = nz // 8
    column_weights((ny, lp, nx), inverse, block, bins, whi, wlo, onehot)

    @pl.loop(0, 3)
    def _(c):
        for p in range(pairs + 2):
            turned = held[:, c, p].reshape(nx, nx).T
            for hf in range(halves):
                first = turned[2 * hf * nz : (2 * hf + 1) * nz]
                second = turned[(2 * hf + 1) * nz : (2 * hf + 2) * nz]
                u[c, hf, 2 * p], u[c, hf, 2 * p + 1] = swap_bit(first, second, 4)

    lane = lax.broadcasted_iota(jnp.int32, (nz, nx), 1)
    last, first_lane = lane % 8 == 7, lane % 8 == 0
    top, bottom = lane == nx - 1, lane == 0

    @pl.loop(0, across + 2)
    def _(x):
        here, dx, dy, dz = [], [], [], []
        for c in range(3):
            v = [u[c, hf, x + 1] for hf in range(2)]
            here.append(v)
            dx.append([u[c, hf, x + 2] - u[c, hf, x] for hf in range(2)])
            dz.append([pltpu.roll(v[hf], nz - 1, 0) - pltpu.roll(v[hf], 1, 0) for hf in range(2)])
            ahead = [pltpu.roll(v[hf], nx - 1, 1) for hf in range(2)]
            behind = [pltpu.roll(v[hf], 1, 1) for hf in range(2)]
            up = [
                jnp.where(last, pltpu.roll(v[1], 7, 1), ahead[0]),
                jnp.where(last, jnp.where(top, 0.0, ahead[0]), ahead[1]),
            ]
            down = [
                jnp.where(first_lane, jnp.where(bottom, 0.0, behind[1]), behind[0]),
                jnp.where(first_lane, pltpu.roll(v[0], nx - 7, 1), behind[1]),
            ]
            dy.append([up[hf] - down[hf] for hf in range(2)])
        for hf in range(2):
            gx, gy, gz = [d[hf] for d in dx], [d[hf] for d in dy], [d[hf] for d in dz]
            s = [gx[0] + gx[0], gy[1] + gy[1], gz[2] + gz[2], gy[0] + gx[1], gz[0] + gx[2], gz[1] + gy[2]]
            mag = tensor_norm(s)
            for c in range(3):
                fields[c, x, hf] = here[c][hf]
            for q, (i, j) in enumerate(PAIRS):
                fields[3 + q, x, hf] = s[q]
                fields[9 + q, x, hf] = here[i][hf] * here[j][hf]
                fields[15 + q, x, hf] = mag * s[q]

    @pl.loop(0, 21)
    def _(k):
        columns = []
        for hf in range(2):
            pair = [fields[k, x, hf] + fields[k, x + 1, hf] for x in range(across + 1)]
            rows = []
            for x in range(across):
                along = pair[x] + pair[x + 1]
                rows.append(pltpu.roll(along, 1, 0) + pltpu.roll(along, nz - 1, 0) + (along + along))
            columns.append(jnp.concatenate(rows, axis=0))
        box = jnp.concatenate(columns, axis=1)
        high = box.astype(jnp.bfloat16)
        low = (box - high.astype(jnp.float32)).astype(jnp.bfloat16)
        dot = functools.partial(jnp.dot, preferred_element_type=jnp.float32)
        filt[k] = dot(high, whi[...]) + (dot(low, whi[...]) + dot(high, wlo[...]))

    sums[...] = jnp.zeros(sums.shape, jnp.float32)

    @pl.loop(0, across * tiles)
    def _(r):
        rows = pl.ds(pl.multiple_of(8 * r, 8), 8)
        for hf in range(2):
            cols = slice(hf * nx, (hf + 1) * nx)
            g = [filt[k, rows, cols] for k in range(21)]
            fmag = 4.0 * tensor_norm(g[3:9])
            lm_total = jnp.zeros((8, nx), jnp.float32)
            mm_total = jnp.zeros((8, nx), jnp.float32)
            for q, (i, j) in enumerate(PAIRS):
                leonard = g[9 + q] - g[i] * g[j]
                model = g[15 + q] - fmag * g[3 + q]
                weighted = model if q < 3 else 2.0 * model
                lm_total += leonard * weighted
                mm_total += model * weighted
                stress[q, hf, rows, :] = leonard
            sums[0, :, cols] += lm_total
            sums[1, :, cols] += mm_total

    @pl.loop(0, 6)
    def _(f):
        for p in range(pairs):
            rows = []
            for hf in range(halves):
                first = stress[f, hf, 2 * p * nz : (2 * p + 1) * nz, :]
                second = stress[f, hf, (2 * p + 1) * nz : (2 * p + 2) * nz, :]
                rows.extend(swap_bit(first, second, 4))
            turned = jnp.concatenate(rows, axis=0).T
            at = pl.ds(pl.multiple_of((f * pairs + p) * 8, 8), 8)
            back[:, at, :] = turned.reshape(n, 8, nx)

    exact = functools.partial(
        lax.dot_general, dimension_numbers=(((1,), (1,)), ((), ())),
        preferred_element_type=jnp.float32, precision=lax.Precision.HIGHEST,
    )
    lm_bins = jnp.sum(exact(sums[0], onehot[...]), axis=0, keepdims=True) * (1.0 / 16.0)
    mm_bins = jnp.sum(exact(sums[1], onehot[...]), axis=0, keepdims=True) * (1.0 / 256.0)
    row = lax.broadcasted_iota(jnp.int32, (8, nx), 0)
    tile = jnp.where(row < 4, lm_bins, mm_bins)
    for p in range(n):
        back[p, 6 * pairs * 8 :, :] = tile


def gather_kernel(n, back, velocity, home, sums, out, beside, near, back_out, back_in, sum_out, sum_in, halo_out, halo_in):
    _, lp, nz, nx = velocity.shape
    a, s = lax.axis_index("px"), lax.axis_index("pz")
    h = n // 2
    rows = back.shape[1] - 8
    greet_all(2, n)
    slot = 2 * lax.rem(s, h) + a
    half = s // h
    remote = functools.partial(pltpu.make_async_remote_copy, device_id_type=MESH)
    halos = [
        remote(velocity, beside, halo_out.at[0], halo_in.at[0], device_id=(1 - a, s)),
        remote(velocity.at[:, lp - 1], near.at[0], halo_out.at[1], halo_in.at[1], device_id=(a, lax.rem(s + 1, n))),
        remote(velocity.at[:, 0], near.at[1], halo_out.at[2], halo_in.at[2], device_id=(a, lax.rem(s + n - 1, n))),
    ]
    for copy in halos:
        copy.start()

    def send(source, dst, core, chip, out_sem, in_sem):
        itself = (core == a) & (chip == s)
        copy = remote(source, dst, out_sem, in_sem, device_id=(core, chip))
        return itself, copy, pltpu.make_async_copy(source, dst, in_sem)

    def sends(p):
        yield send(back.at[p], home.at[slot], half, p, back_out.at[p], back_in.at[slot])
        yield send(back.at[p, pl.ds(rows, 8)], sums.at[slot], 1 - half, p, sum_out.at[p], sum_in.at[slot])

    @pl.loop(0, n)
    def _(i):
        for itself, copy, here in sends(lax.rem(s + i, n)):
            pl.when(itself)(here.start)
            pl.when(jnp.logical_not(itself))(copy.start)

    for copy in halos:
        copy.wait()
    lane = lax.broadcasted_iota(jnp.int32, (nz, nx), 1)
    has_below = (s > 0).astype(jnp.float32)
    has_above = (s < n - 1).astype(jnp.float32)

    def plane(y, ups, downs):
        dx, dy, dz = [], [], []
        for c in range(3):
            v, side = velocity[c, y], beside[c, y]
            ahead = jnp.where(lane == nx - 1, pltpu.roll(side, nx - 1, 1), pltpu.roll(v, nx - 1, 1))
            behind = jnp.where(lane == 0, pltpu.roll(side, 1, 1), pltpu.roll(v, 1, 1))
            dx.append(ahead - behind)
            dz.append(pltpu.roll(v, nz - 1, 0) - pltpu.roll(v, 1, 0))
            dy.append(ups[c] - downs[c])
        out[y] = tensor_norm(strain_of(dx, dy, dz))

    line = [near[0, c] * has_below for c in range(3)]
    plane(0, [velocity[c, 1] for c in range(3)], line)
    line = [near[1, c] * has_above for c in range(3)]
    plane(lp - 1, line, [velocity[c, lp - 2] for c in range(3)])

    @pl.loop(1, lp - 1)
    def _(y):
        plane(y, [velocity[c, y + 1] for c in range(3)], [velocity[c, y - 1] for c in range(3)])

    @pl.loop(0, n)
    def _(p):
        pltpu.make_async_copy(back.at[0], home.at[p], back_in.at[p]).wait()
        pltpu.make_async_copy(back.at[0, pl.ds(rows, 8)], sums.at[p], sum_in.at[p]).wait()
        for itself, copy, here in sends(p):
            pl.when(jnp.logical_not(itself))(copy.wait_send)


def finish_kernel(dims, cells, chip, home, sums, magnitude, bins, leonard, viscosity, coefficient):
    n, pairs, lp, nz, nx = dims
    ny, groups = n * lp, nx // nz
    steps = lp // groups
    rows = 6 * pairs * 8
    total = home[0, rows:, :] + sums[0]
    for p in range(1, n):
        total = total + (home[p, rows:, :] + sums[p])
    numer, denom = total[0:1, :], total[4:5, :]
    per_bin = numer / jnp.maximum(denom, jnp.float32(cells))
    exact = functools.partial(
        lax.dot_general, preferred_element_type=jnp.float32, precision=lax.Precision.HIGHEST
    )
    label = jnp.broadcast_to(bins[...].astype(jnp.float32), (nx, ny))
    kind = lax.broadcasted_iota(jnp.int32, (nx, ny), 0).astype(jnp.float32)
    onehot = (label == kind).astype(jnp.float32)
    table = jnp.broadcast_to(per_bin, (nx, nx))
    coefficient[...] = exact(table[0:8], onehot, (((1,), (0,)), ((), ())))[0:1, :]
    mine = jnp.zeros((nx, lp), jnp.float32)
    for s in range(n):
        mine = jnp.where(chip[0] == s, onehot[:, s * lp : (s + 1) * lp], mine)
    spread = exact(mine, table, (((0,), (1,)), ((), ())))
    for y in range(lp):
        viscosity[y] = spread[y : y + 1, :] * magnitude[y]

    @pl.loop(0, 6)
    def _(f):
        for q in range(steps):
            at = pl.ds(f * pairs * 8 + q, nx // n, stride=steps)
            turned = jnp.concatenate([home[p, at, :] for p in range(n)], axis=0).T
            for g in range(groups):
                leonard[f, g * steps + q] = turned[g * nz : (g + 1) * nz]


def by_strips(velocity, filter_inverse, filter_block, plane_bin, n):
    _, lp, nz, nx = velocity.shape
    ny, h = n * lp, n // 2
    pairs = nx // h // 4
    dims = (n, pairs, lp, nz, nx)
    steps = lp // (nx // nz)
    chip = lax.axis_index("pz").astype(jnp.int32).reshape(1)
    block = filter_block.reshape(1, ny)
    bins = plane_bin.reshape(1, ny)
    vmem = pl.BlockSpec(memory_space=pltpu.VMEM)
    smem = pl.BlockSpec(memory_space=pltpu.SMEM)
    f32 = functools.partial(jax.ShapeDtypeStruct, dtype=jnp.float32)
    dma = pltpu.SemaphoreType.DMA
    cells = 2 * pairs * nz

    packed = pl.pallas_call(
        functools.partial(pack_kernel, (lp, nz, nx)),
        out_shape=f32((3, nx * steps, nx)),
        in_specs=[vmem],
        out_specs=vmem,
    )(velocity)
    held = pl.pallas_call(
        functools.partial(spread_kernel, (n, h, pairs)),
        out_shape=f32((n, 3, pairs + 2, 8, nx)),
        in_specs=[vmem],
        out_specs=vmem,
        scratch_shapes=[dma((h, 2)), dma((h,)), dma((h,)), dma((n,)), dma((n,)), dma((n,)), dma((n,))],
        compiler_params=pltpu.CompilerParams(collective_id=0, has_side_effects=True),
    )(packed.reshape(3, nx * steps // 8, 8, nx))
    back = pl.pallas_call(
        functools.partial(strip_kernel, dims),
        out_shape=f32((n, 6 * pairs * 8 + 8, nx)),
        in_specs=[vmem] * 4,
        out_specs=vmem,
        scratch_shapes=[
            pltpu.VMEM((3, 2, 2 * pairs + 4, nz, nx), jnp.float32),
            pltpu.VMEM((21, 2 * pairs + 2, 2, nz, nx), jnp.float32),
            pltpu.VMEM((21, cells, ny), jnp.float32),
            pltpu.VMEM((6, 2, cells, nx), jnp.float32),
            pltpu.VMEM((ny, ny), jnp.bfloat16),
            pltpu.VMEM((ny, ny), jnp.bfloat16),
            pltpu.VMEM((nx, ny), jnp.float32),
            pltpu.VMEM((2, 8, ny), jnp.float32),
        ],
        compiler_params=pltpu.CompilerParams(vmem_limit_bytes=60 * 1024 * 1024),
    )(held, filter_inverse, block, bins)
    home, sums, magnitude = pl.pallas_call(
        functools.partial(gather_kernel, n),
        out_shape=(f32(back.shape), f32((n, 8, nx)), f32((lp, nz, nx))),
        in_specs=[vmem] * 2,
        out_specs=(vmem,) * 3,
        scratch_shapes=[
            pltpu.VMEM((3, lp, nz, nx), jnp.float32),
            pltpu.VMEM((2, 3, nz, nx), jnp.float32),
            dma((n,)),
            dma((n,)),
            dma((n,)),
            dma((n,)),
            dma((3,)),
            dma((3,)),
        ],
        compiler_params=pltpu.CompilerParams(collective_id=1, has_side_effects=True),
    )(back, velocity)
    leonard, viscosity, coefficient = pl.pallas_call(
        functools.partial(finish_kernel, dims, 2 * nx * nz),
        out_shape=(f32((6, lp, nz, nx)), f32((lp, nz, nx)), f32((1, ny))),
        in_specs=[smem] + [vmem] * 4,
        out_specs=(vmem,) * 3,
    )(chip, home, sums, magnitude, bins)
    return (leonard, viscosity, coefficient.reshape(ny))


def by_blocks(velocity, filter_inverse, filter_block, plane_bin):
    _, lp, nz, nx = velocity.shape
    n = lax.axis_size("pz")
    m = lax.axis_size("px")
    ny, zs = n * lp, nz // n
    win = zs + 4

    same = (filter_block[:, None] == filter_block[None, :]).astype(jnp.float32)
    masked = filter_inverse * same
    weights = masked / jnp.sum(masked, axis=1, keepdims=True)
    onehot = (plane_bin[:, None] == jnp.arange(nx, dtype=jnp.int32)[None, :]).astype(jnp.float32)

    right = lax.ppermute(velocity, "px", [((i + 1) % m, i) for i in range(m)])
    left = right if m == 2 else lax.ppermute(velocity, "px", [(i, (i + 1) % m) for i in range(m)])
    below = lax.ppermute(velocity[:, -1:], "pz", [(i, i + 1) for i in range(n - 1)])
    above = lax.ppermute(velocity[:, :1], "pz", [(i + 1, i) for i in range(n - 1)])
    magnitude = pl.pallas_call(
        magnitude_kernel,
        out_shape=jax.ShapeDtypeStruct((lp, nz, nx), jnp.float32),
        cost_estimate=pl.CostEstimate(flops=60 * lp * nz * nx, bytes_accessed=40 * lp * nz * nx, transcendentals=0),
    )(velocity, right, left, below, above)
    turned = jnp.transpose(velocity, (0, 2, 1, 3))
    turned = jnp.concatenate([turned[:, -2:], turned, turned[:, :2]], axis=1)
    sent = jnp.stack([turned[:, t * zs : t * zs + win] for t in range(n)])
    own = lax.all_to_all(sent, "pz", split_axis=0, concat_axis=0, tiled=True)
    ahead = lax.ppermute(own, "px", [((i + 1) % m, i) for i in range(m)])
    behind = lax.ppermute(own, "px", [(i, (i + 1) % m) for i in range(m)])
    blocks = (own, ahead, behind)

    rows = 6 * zs * lp
    back = pl.pallas_call(
        functools.partial(column_kernel, (n, win, lp, nx), fill_from_blocks, len(blocks)),
        out_shape=jax.ShapeDtypeStruct((n, rows + 8, nx), jnp.float32),
        in_specs=[pl.BlockSpec(memory_space=pltpu.VMEM)] * 5,
        out_specs=pl.BlockSpec(memory_space=pltpu.VMEM),
        scratch_shapes=[
            pltpu.VMEM((3, win, ny + 16, 2 * nx), jnp.float32),
            pltpu.VMEM((21, ny, zs * nx), jnp.bfloat16),
            pltpu.VMEM((21, ny, zs * nx), jnp.bfloat16),
            pltpu.VMEM((21, ny, zs * nx), jnp.float32),
            pltpu.VMEM((ny, nx), jnp.float32),
            pltpu.VMEM((ny, nx), jnp.float32),
            pltpu.VMEM((ny, ny), jnp.bfloat16),
            pltpu.VMEM((ny, ny), jnp.bfloat16),
        ],
        compiler_params=pltpu.CompilerParams(vmem_limit_bytes=60 * 1024 * 1024),
    )(*blocks, weights, onehot)

    home = lax.all_to_all(back, "pz", split_axis=0, concat_axis=0, tiled=True)
    totals = lax.psum(jnp.sum(home[:, rows:], axis=0), "px")
    stress = home[:, :rows].reshape(n, 6, zs, lp, nx)
    leonard = jnp.transpose(stress, (1, 3, 0, 2, 4)).reshape(6, lp, nz, nx)
    numer, denom = totals[0, :NBIN], totals[4, :NBIN]
    cells = nx * m * nz
    per_bin = numer / jnp.maximum(denom, jnp.float32(cells))
    coefficient = jnp.dot(onehot[:, :NBIN], per_bin, precision=lax.Precision.HIGHEST)
    local_coef = lax.dynamic_slice_in_dim(coefficient, lax.axis_index("pz") * lp, lp, 0)
    viscosity = local_coef[:, None, None] * magnitude
    return (leonard, viscosity, coefficient)


def local(*arrays):
    _, lp, nz, nx = arrays[0].shape
    n, m = lax.axis_size("pz"), lax.axis_size("px")
    groups = nx // nz
    fits = m == 2 and n % 2 == 0 and 8 * n == nx and groups * nz == nx and lp == 16 and groups == 4
    if fits:
        return by_strips(*arrays, n)
    return by_blocks(*arrays)


def solution(mesh):
    return jax.shard_map(
        local,
        mesh=mesh,
        in_specs=(P(None, "pz", None, "px"), P(), P(), P()),
        out_specs=(P(None, "pz", None, "px"), P("pz", None, "px"), P()),
        check_vma=False,
    )
```

```python
import functools

import jax
import jax.numpy as jnp
from jax import lax
from jax.experimental import pallas as pl
from jax.experimental.pallas import tpu as pltpu
from jax.sharding import PartitionSpec as P

NBIN = 64
MESH = pl.DeviceIdType.MESH
PAIRS = ((0, 0), (1, 1), (2, 2), (0, 1), (0, 2), (1, 2))


def tensor_norm(s):
    diag = s[0] * s[0] + s[1] * s[1] + s[2] * s[2]
    off = s[3] * s[3] + s[4] * s[4] + s[5] * s[5]
    return jnp.sqrt(2.0 * diag + 4.0 * off)


def strain_of(dx, dy, dz):
    return [
        dx[0] * 0.5,
        dy[1] * 0.5,
        dz[2] * 0.5,
        0.25 * (dy[0] + dx[1]),
        0.25 * (dz[0] + dx[2]),
        0.25 * (dz[1] + dy[2]),
    ]


def fill_from_blocks(dims, ext, own, right, left):
    n, win, lp, nx = dims
    lane = lax.broadcasted_iota(jnp.int32, (lp, nx), 1)
    from_right = lane < nx // 2

    @pl.loop(0, n)
    def _(p):
        rows = pl.ds(pl.multiple_of(8 + p * lp, 8), lp)
        for c in range(3):
            for z in range(win):
                ext[c, z, rows, 0:nx] = own[p, c, z]
                ext[c, z, rows, nx : 2 * nx] = jnp.where(from_right, right[p, c, z], left[p, c, z])


def column_kernel(dims, fill, sources, *refs):
    n, win, lp, nx = dims
    blocks, refs = refs[:sources], refs[sources:]
    weights, onehot, back, ext, bhi, blo, filt, lms, mms, whi, wlo = refs
    zs = win - 4
    ny = n * lp
    lanes = 2 * nx
    heavy = weights[...].astype(jnp.bfloat16)
    whi[...] = heavy
    wlo[...] = (weights[...] - heavy.astype(jnp.float32)).astype(jnp.bfloat16)

    zero = jnp.zeros((8, lanes), jnp.float32)
    for c in range(3):
        for z in range(win):
            ext[c, z, 0:8, :] = zero
            ext[c, z, ny + 8 : ny + 16, :] = zero
    fill(dims, ext, *blocks)

    @pl.loop(0, n)
    def _(p):
        base = pl.multiple_of(p * lp, 8)
        u = [[ext[c, z, pl.ds(base + 8, lp), :] for z in range(win)] for c in range(3)]
        boxes = [[None] * 21 for _ in range(zs)]
        for z in range(1, win - 1):
            v = [u[c][z] for c in range(3)]
            dx, dy, dz = [], [], []
            for c in range(3):
                dx.append(pltpu.roll(v[c], lanes - 1, 1) - pltpu.roll(v[c], 1, 1))
                tall = ext[c, z, pl.ds(base, lp + 16), :]
                dy.append(tall[9 : 9 + lp] - tall[7 : 7 + lp])
                dz.append(u[c][z + 1] - u[c][z - 1])
            s = strain_of(dx, dy, dz)
            mag = tensor_norm(s)
            fields = v + s + [v[i] * v[j] for i, j in PAIRS] + [mag * t for t in s]
            for o in range(zs):
                step = z - (o + 2)
                if -1 <= step <= 1:
                    for k in range(21):
                        term = fields[k] if step else 2.0 * fields[k]
                        boxes[o][k] = term if boxes[o][k] is None else boxes[o][k] + term
        for o in range(zs):
            for k in range(21):
                f = boxes[o][k]
                box = (pltpu.roll(f, 1, 1) + pltpu.roll(f, lanes - 1, 1) + 2.0 * f)[:, :nx] * 0.0625
                high = box.astype(jnp.bfloat16)
                cols = slice(o * nx, (o + 1) * nx)
                bhi[k, pl.ds(base, lp), cols] = high
                blo[k, pl.ds(base, lp), cols] = (box - high.astype(jnp.float32)).astype(jnp.bfloat16)

    @pl.loop(0, 21)
    def _(k):
        dot = functools.partial(jnp.dot, preferred_element_type=jnp.float32)
        filt[k] = dot(whi[...], bhi[k]) + (dot(whi[...], blo[k]) + dot(wlo[...], bhi[k]))

    @pl.loop(0, n)
    def _(p):
        base = pl.multiple_of(p * lp, 8)
        lm_total = jnp.zeros((lp, nx), jnp.float32)
        mm_total = jnp.zeros((lp, nx), jnp.float32)
        for o in range(zs):
            g = [filt[k, pl.ds(base, lp), o * nx : (o + 1) * nx] for k in range(21)]
            fmag = 4.0 * tensor_norm(g[3:9])
            for q, (i, j) in enumerate(PAIRS):
                leonard = g[9 + q] - g[i] * g[j]
                model = g[15 + q] - fmag * g[3 + q]
                weighted = model if q < 3 else 2.0 * model
                lm_total += leonard * weighted
                mm_total += model * weighted
                back[p, (q * zs + o) * lp : (q * zs + o + 1) * lp, :] = leonard
        lms[pl.ds(base, lp), :] = lm_total
        mms[pl.ds(base, lp), :] = mm_total

    ones = jnp.ones((8, nx), jnp.float32)
    exact = functools.partial(
        lax.dot_general, preferred_element_type=jnp.float32, precision=lax.Precision.HIGHEST
    )
    totals = []
    for part in (lms, mms):
        planes = exact(ones, part[...], (((1,), (1,)), ((), ())))
        totals.append(exact(planes, onehot[...], (((1,), (0,)), ((), ()))))
    row = lax.broadcasted_iota(jnp.int32, (8, onehot.shape[1]), 0)
    tile = jnp.where(row < 4, totals[0], totals[1])
    for p in range(n):
        back[p, 6 * zs * lp :, :] = tile


def greet_all(m, n):
    me = lax.axis_index("px") * n + lax.axis_index("pz")
    barrier = pltpu.get_barrier_semaphore()

    @pl.loop(1, m * n)
    def _(step):
        peer = lax.rem(me + step, m * n)
        pl.semaphore_signal(barrier, inc=1, device_id=(peer // n, lax.rem(peer, n)), device_id_type=MESH)

    pl.semaphore_wait(barrier, m * n - 1)


def magnitude_kernel(centre, right, left, below, above, out):
    _, lp, nz, nx = centre.shape
    lane = lax.broadcasted_iota(jnp.int32, (nz, nx), 1)
    for y in range(lp):
        v = [centre[c, y] for c in range(3)]
        dx, dy, dz = [], [], []
        for c in range(3):
            ahead = jnp.where(lane == nx - 1, pltpu.roll(right[c, y], nx - 1, 1), pltpu.roll(v[c], nx - 1, 1))
            behind = jnp.where(lane == 0, pltpu.roll(left[c, y], 1, 1), pltpu.roll(v[c], 1, 1))
            dx.append(ahead - behind)
            dz.append(pltpu.roll(v[c], nz - 1, 0) - pltpu.roll(v[c], 1, 0))
            up = centre[c, y + 1] if y + 1 < lp else above[c, 0]
            down = centre[c, y - 1] if y else below[c, 0]
            dy.append(up - down)
        out[y] = tensor_norm(strain_of(dx, dy, dz))


def swap_bit(first, second, bit):
    nx = first.shape[-1]
    low = (lax.broadcasted_iota(jnp.int32, first.shape, 1) & bit) == 0
    return (
        jnp.where(low, first, pltpu.roll(second, bit, 1)),
        jnp.where(low, pltpu.roll(first, nx - bit, 1), second),
    )


def pack_kernel(dims, velocity, packed):
    lp, nz, nx = dims
    groups = nx // nz
    steps = lp // groups

    @pl.loop(0, 3)
    def _(c):
        for q in range(steps):
            rows = jnp.concatenate([velocity[c, g * steps + q] for g in range(groups)], axis=0)
            packed[c, pl.ds(q, nx, stride=steps), :] = rows.T


def plane_order(shape, lp, nx, dim):
    at = lax.broadcasted_iota(jnp.int32, shape, dim)
    return (at % nx) // 8 * lp + at // nx * 8 + at % 8


def column_weights(dims, inverse, block, bins, whi, wlo, onehot):
    ny, lp, nx = dims
    label = jnp.broadcast_to(block[...].astype(jnp.float32), (ny, ny))
    masked = jnp.where(label == label.T, inverse[...], 0.0)
    weights = masked / jnp.sum(masked, axis=1, keepdims=True) * 0.0625
    order = plane_order((ny, ny), lp, nx, 0) == lax.broadcasted_iota(jnp.int32, (ny, ny), 1)
    order = order.astype(jnp.float32).astype(jnp.bfloat16)
    across = functools.partial(
        lax.dot_general, dimension_numbers=(((1,), (1,)), ((), ())), preferred_element_type=jnp.float32
    )

    def placed(part):
        turned = across(order, part).astype(jnp.bfloat16)
        return across(turned, order).astype(jnp.bfloat16)

    heavy = weights.astype(jnp.bfloat16)
    whi[...] = placed(heavy)
    wlo[...] = placed((weights - heavy.astype(jnp.float32)).astype(jnp.bfloat16))
    label = jnp.broadcast_to(bins[...], (nx, ny))
    hot = (label == lax.broadcasted_iota(jnp.int32, (nx, ny), 0)).astype(jnp.float32)
    onehot[...] = across(hot.astype(jnp.bfloat16), order)


def flip_bits(value, mask, count):
    out = 0
    for bit in range(count):
        digit = lax.rem(value // (1 << bit), 2)
        out = out + (1 << bit) * ((1 - digit) if mask >> bit & 1 else digit)
    return out


def plane_magnitudes(velocity, beside, near, out, has_below, has_above):
    _, lp, nz, nx = velocity.shape
    lane = lax.broadcasted_iota(jnp.int32, (nz, nx), 1)

    def plane(y, ups, downs):
        dx, dy, dz = [], [], []
        for c in range(3):
            v, side = velocity[c, y], beside[c, y]
            ahead = jnp.where(lane == nx - 1, pltpu.roll(side, nx - 1, 1), pltpu.roll(v, nx - 1, 1))
            behind = jnp.where(lane == 0, pltpu.roll(side, 1, 1), pltpu.roll(v, 1, 1))
            dx.append(ahead - behind)
            dz.append(pltpu.roll(v, nz - 1, 0) - pltpu.roll(v, 1, 0))
            dy.append(ups[c] - downs[c])
        out[y] = tensor_norm(strain_of(dx, dy, dz))

    line = [near[0, c] * has_below for c in range(3)]
    plane(0, [velocity[c, 1] for c in range(3)], line)
    line = [near[1, c] * has_above for c in range(3)]
    plane(lp - 1, line, [velocity[c, lp - 2] for c in range(3)])

    @pl.loop(1, lp - 1)
    def _(y):
        plane(y, [velocity[c, y + 1] for c in range(3)], [velocity[c, y - 1] for c in range(3)])


def unpack_pair(held, u, slot, nz, nx):
    @pl.loop(0, 3)
    def _(c):
        turned = held[:, c, slot].reshape(nx, nx).T
        for hf in range(2):
            first = turned[2 * hf * nz : (2 * hf + 1) * nz]
            second = turned[(2 * hf + 1) * nz : (2 * hf + 2) * nz]
            u[c, hf, 2 * slot], u[c, hf, 2 * slot + 1] = swap_bit(first, second, 4)


def field_columns(u, fields, start, count, nz, nx):
    lane = lax.broadcasted_iota(jnp.int32, (nz, nx), 1)
    last, first_lane = lane % 8 == 7, lane % 8 == 0
    top, bottom = lane == nx - 1, lane == 0

    @pl.loop(0, count)
    def _(i):
        x = start + i
        here, dx, dy, dz = [], [], [], []
        for c in range(3):
            v = [u[c, hf, x] for hf in range(2)]
            here.append(v)
            dx.append([u[c, hf, x + 1] - u[c, hf, x - 1] for hf in range(2)])
            dz.append([pltpu.roll(v[hf], nz - 1, 0) - pltpu.roll(v[hf], 1, 0) for hf in range(2)])
            ahead = [pltpu.roll(v[hf], nx - 1, 1) for hf in range(2)]
            behind = [pltpu.roll(v[hf], 1, 1) for hf in range(2)]
            up = [
                jnp.where(last, pltpu.roll(v[1], 7, 1), ahead[0]),
                jnp.where(last, jnp.where(top, 0.0, ahead[0]), ahead[1]),
            ]
            down = [
                jnp.where(first_lane, jnp.where(bottom, 0.0, behind[1]), behind[0]),
                jnp.where(first_lane, pltpu.roll(v[0], nx - 7, 1), behind[1]),
            ]
            dy.append([up[hf] - down[hf] for hf in range(2)])
        for hf in range(2):
            gx, gy, gz = [d[hf] for d in dx], [d[hf] for d in dy], [d[hf] for d in dz]
            s = [gx[0] + gx[0], gy[1] + gy[1], gz[2] + gz[2], gy[0] + gx[1], gz[0] + gx[2], gz[1] + gy[2]]
            mag = tensor_norm(s)
            for c in range(3):
                fields[c, x, hf] = here[c][hf]
            for q, (i, j) in enumerate(PAIRS):
                fields[3 + q, x, hf] = s[q]
                fields[9 + q, x, hf] = here[i][hf] * here[j][hf]
                fields[15 + q, x, hf] = mag * s[q]


def filter_pair(fields, start, high, low, filt, whi, wlo, nz):
    cells = 2 * nz

    @pl.loop(0, 21)
    def _(k):
        columns = []
        for hf in range(2):
            f = [fields[k, start + i, hf] for i in range(4)]
            pair = [f[i] + f[i + 1] for i in range(3)]
            rows = []
            for i in range(2):
                along = pair[i] + pair[i + 1]
                rows.append(pltpu.roll(along, 1, 0) + pltpu.roll(along, nz - 1, 0) + (along + along))
            columns.append(jnp.concatenate(rows, axis=0))
        box = jnp.concatenate(columns, axis=1)
        heavy = box.astype(jnp.bfloat16)
        at = pl.ds(pl.multiple_of(k * cells, cells), cells)
        high[at, :] = heavy
        low[at, :] = (box - heavy.astype(jnp.float32)).astype(jnp.bfloat16)

    @pl.loop(0, 3)
    def _(b):
        dot = functools.partial(jnp.dot, preferred_element_type=jnp.float32)
        at = pl.ds(pl.multiple_of(b * 7 * cells, cells), 7 * cells)
        head, rest = high[at, :], low[at, :]
        filt[at, :] = dot(head, whi[...]) + (dot(rest, whi[...]) + dot(head, wlo[...]))


def stress_pair(filt, stress, sums, nz, nx):
    cells = 2 * nz

    @pl.loop(0, cells // 8)
    def _(r):
        base = pl.multiple_of(8 * r, 8)
        for hf in range(2):
            cols = slice(hf * nx, (hf + 1) * nx)
            g = [filt[pl.ds(base + k * cells, 8), cols] for k in range(21)]
            fmag = 4.0 * tensor_norm(g[3:9])
            lm_total = jnp.zeros((8, nx), jnp.float32)
            mm_total = jnp.zeros((8, nx), jnp.float32)
            for q, (i, j) in enumerate(PAIRS):
                leonard = g[9 + q] - g[i] * g[j]
                model = g[15 + q] - fmag * g[3 + q]
                weighted = model if q < 3 else 2.0 * model
                lm_total += leonard * weighted
                mm_total += model * weighted
                stress[q, hf, pl.ds(base, 8), :] = leonard
            sums[0, :, cols] += lm_total
            sums[1, :, cols] += mm_total


def flow_kernel(
    dims, packed, velocity, inverse, block, bins, home, totals, magnitude,
    held, u, fields, high, low, filt, stress, back, whi, wlo, onehot, sums, tile, beside, near,
    main_out, edge_out, pass_out, back_out, sum_out, halo_out,
    main_in, edge_in, pass_in, back_in, sum_in, halo_in,
):
    n, pairs, lp, nz, nx = dims
    ny, h = n * lp, n // 2
    bits = n.bit_length() - 1
    whole = 2 * pairs
    a, s = lax.axis_index("px"), lax.axis_index("pz")
    remote = functools.partial(pltpu.make_async_remote_copy, device_id_type=MESH)
    greet_all(2, n)

    def send(source, dst, core, chip, out_sem, in_sem):
        itself = (core == a) & (chip == s)
        copy = remote(source, dst, out_sem, in_sem, device_id=(core, chip))
        return itself, copy, pltpu.make_async_copy(source, dst, in_sem)

    def start(moves):
        for itself, copy, here in moves:
            pl.when(itself)(here.start)
            pl.when(jnp.logical_not(itself))(copy.start)

    def drain(moves):
        for itself, copy, here in moves:
            pl.when(jnp.logical_not(itself))(copy.wait_send)

    def edges(i):
        chip = h * a + i
        yield send(packed.at[:, pl.ds(whole * i + whole - 1, 1)], held.at[s, :, 0:1], 0, lax.rem(chip + 1, n), edge_out.at[0, i], edge_in.at[s])
        yield send(packed.at[:, pl.ds(whole * i, 1)], held.at[s, :, pairs + 1 : pairs + 2], 1, lax.rem(chip + n - 1, n), edge_out.at[1, i], edge_in.at[s])

    def mains(i, m):
        for core in range(2):
            own = m if core == 0 else pairs - 1 - m
            source = packed.at[:, pl.ds(whole * i + pairs * core + own, 1)]
            yield send(source, held.at[s, :, own + 1 : own + 2], core, h * a + i, main_out.at[m, core, i], main_in.at[m, s])

    @pl.loop(0, h)
    def _(r):
        start(edges(lax.rem(s + r, h)))

    for m in range(pairs):
        @pl.loop(0, h)
        def _(r):
            start(mains(lax.rem(s + r, h), m))

    halos = [
        remote(velocity, beside, halo_out.at[0], halo_in.at[0], device_id=(1 - a, s)),
        remote(velocity.at[:, lp - 1], near.at[0], halo_out.at[1], halo_in.at[1], device_id=(a, lax.rem(s + 1, n))),
        remote(velocity.at[:, 0], near.at[1], halo_out.at[2], halo_in.at[2], device_id=(a, lax.rem(s + n - 1, n))),
    ]
    for copy in halos:
        copy.start()

    column_weights((ny, lp, nx), inverse, block, bins, whi, wlo, onehot)
    sums[...] = jnp.zeros(sums.shape, jnp.float32)

    def slot_of(m):
        return 1 + m + a * (pairs - 1 - 2 * m)

    def forward(p):
        return remote(
            held.at[p, :, pl.ds(slot_of(pairs - 1), 1)], held.at[p, :, pl.ds((pairs + 1) * a, 1)],
            pass_out.at[p], pass_in.at[p], device_id=(1 - a, s),
        )

    def await_pair(sems, p):
        pltpu.make_async_copy(packed.at[:, 0:1], held.at[p, :, 0:1], sems).wait()

    half = s // h
    mine = 2 * lax.rem(s, h) + a

    def returns(j, d):
        pair = slot_of(j) - 1
        return [send(back.at[j, d], home.at[mine, :, pair], half, d, back_out.at[j, d], back_in.at[j, mine])]

    def column(j):
        q = slot_of(j)
        if j == 0:
            field_columns(u, fields, 2 * q - 1, 4, nz, nx)
        else:
            field_columns(u, fields, 2 * q + 1 - 2 * a, 2, nz, nx)
        filter_pair(fields, 2 * q - 1, high, low, filt, whi, wlo, nz)
        stress_pair(filt, stress, sums, nz, nx)

        @pl.loop(0, 6)
        def _(f):
            rows = []
            for hf in range(2):
                rows.extend(swap_bit(stress[f, hf, 0:nz, :], stress[f, hf, nz : 2 * nz, :], 4))
            turned = jnp.concatenate(rows, axis=0).T
            back[j, :, f] = turned.reshape(n, 8, nx)

        for r in range(n):
            mask = (r % 2) * h + r // 2
            start(returns(j, flip_bits(s, mask ^ h, bits)))

    @pl.loop(0, n)
    def _(p):
        await_pair(edge_in.at[p], p)
        await_pair(main_in.at[0, p], p)
        await_pair(main_in.at[1, p], p)

    for m in range(-1, 2):
        unpack_pair(held, u, slot_of(m), nz, nx)
    column(0)
    for j in range(1, pairs):
        if j + 1 < pairs:
            @pl.loop(0, n)
            def _(p):
                await_pair(main_in.at[j + 1, p], p)
                if j + 2 == pairs:
                    forward(p).start()
        else:
            @pl.loop(0, n)
            def _(p):
                forward(p).wait()
        unpack_pair(held, u, slot_of(j + 1), nz, nx)
        column(j)

    exact = functools.partial(
        lax.dot_general, dimension_numbers=(((1,), (1,)), ((), ())),
        preferred_element_type=jnp.float32, precision=lax.Precision.HIGHEST,
    )
    lm_bins = jnp.sum(exact(sums[0], onehot[...]), axis=0, keepdims=True) * (1.0 / 16.0)
    mm_bins = jnp.sum(exact(sums[1], onehot[...]), axis=0, keepdims=True) * (1.0 / 256.0)
    row = lax.broadcasted_iota(jnp.int32, (8, nx), 0)
    tile[...] = jnp.where(row < 4, lm_bins, mm_bins)
    me = a * n + s

    def share(t):
        return [send(tile, totals.at[me], t // n, lax.rem(t, n), sum_out.at[t], sum_in.at[me])]

    @pl.loop(0, 2 * n)
    def _(r):
        start(share(lax.rem(me + r, 2 * n)))

    for copy in halos:
        copy.wait()
    plane_magnitudes(velocity, beside, near, magnitude, (s > 0).astype(jnp.float32), (s < n - 1).astype(jnp.float32))

    @pl.loop(0, h)
    def _(i):
        drain(edges(i))
        for m in range(pairs):
            drain(mains(i, m))

    @pl.loop(0, n)
    def _(p):
        for j in range(pairs):
            pltpu.make_async_copy(back.at[0, 0], home.at[p, :, 0], back_in.at[j, p]).wait()
            drain(returns(j, p))

    @pl.loop(0, 2 * n)
    def _(t):
        pltpu.make_async_copy(tile, totals.at[t], sum_in.at[t]).wait()
        drain(share(t))


def finish_kernel(dims, cells, chip, home, sums, magnitude, bins, leonard, viscosity, coefficient):
    n, pairs, lp, nz, nx = dims
    ny, groups = n * lp, nx // nz
    steps = lp // groups
    total = sums[0]
    for p in range(1, 2 * n):
        total = total + sums[p]
    numer, denom = total[0:1, :], total[4:5, :]
    per_bin = numer / jnp.maximum(denom, jnp.float32(cells))
    exact = functools.partial(
        lax.dot_general, preferred_element_type=jnp.float32, precision=lax.Precision.HIGHEST
    )
    label = jnp.broadcast_to(bins[...].astype(jnp.float32), (nx, ny))
    kind = lax.broadcasted_iota(jnp.int32, (nx, ny), 0).astype(jnp.float32)
    onehot = (label == kind).astype(jnp.float32)
    table = jnp.broadcast_to(per_bin, (nx, nx))
    coefficient[...] = exact(table[0:8], onehot, (((1,), (0,)), ((), ())))[0:1, :]
    mine = jnp.zeros((nx, lp), jnp.float32)
    for s in range(n):
        mine = jnp.where(chip[0] == s, onehot[:, s * lp : (s + 1) * lp], mine)
    spread = exact(mine, table, (((0,), (1,)), ((), ())))
    for y in range(lp):
        viscosity[y] = spread[y : y + 1, :] * magnitude[y]

    @pl.loop(0, 6)
    def _(f):
        for q in range(steps):
            at = pl.ds(f * pairs * 8 + q, nx // n, stride=steps)
            turned = jnp.concatenate([home[p, at, :] for p in range(n)], axis=0).T
            for g in range(groups):
                leonard[f, g * steps + q] = turned[g * nz : (g + 1) * nz]


def by_strips(velocity, filter_inverse, filter_block, plane_bin, n):
    _, lp, nz, nx = velocity.shape
    ny, h = n * lp, n // 2
    pairs = nx // h // 4
    dims = (n, pairs, lp, nz, nx)
    steps = lp // (nx // nz)
    chip = lax.axis_index("pz").astype(jnp.int32).reshape(1)
    block = filter_block.reshape(1, ny)
    bins = plane_bin.reshape(1, ny)
    vmem = pl.BlockSpec(memory_space=pltpu.VMEM)
    smem = pl.BlockSpec(memory_space=pltpu.SMEM)
    f32 = functools.partial(jax.ShapeDtypeStruct, dtype=jnp.float32)
    dma = pltpu.SemaphoreType.DMA

    packed = pl.pallas_call(
        functools.partial(pack_kernel, (lp, nz, nx)),
        out_shape=f32((3, nx * steps, nx)),
        in_specs=[vmem],
        out_specs=vmem,
    )(velocity)
    room = functools.partial(pltpu.VMEM, dtype=jnp.float32)
    home, sums, magnitude = pl.pallas_call(
        functools.partial(flow_kernel, dims),
        out_shape=(f32((n, 6, pairs, 8, nx)), f32((2 * n, 8, nx)), f32((lp, nz, nx))),
        in_specs=[vmem] * 5,
        out_specs=(vmem,) * 3,
        scratch_shapes=[
            room((n, 3, pairs + 2, 8, nx)),
            room((3, 2, 2 * pairs + 4, nz, nx)),
            room((21, 2 * pairs + 4, 2, nz, nx)),
            pltpu.VMEM((21 * 2 * nz, ny), jnp.bfloat16),
            pltpu.VMEM((21 * 2 * nz, ny), jnp.bfloat16),
            room((21 * 2 * nz, ny)),
            room((6, 2, 2 * nz, nx)),
            room((pairs, n, 6, 8, nx)),
            pltpu.VMEM((ny, ny), jnp.bfloat16),
            pltpu.VMEM((ny, ny), jnp.bfloat16),
            room((nx, ny)),
            room((2, 8, ny)),
            room((8, nx)),
            room((3, lp, nz, nx)),
            room((2, 3, nz, nx)),
            dma((pairs, 2, h)),
            dma((2, h)),
            dma((n,)),
            dma((pairs, n)),
            dma((2 * n,)),
            dma((3,)),
            dma((pairs, n)),
            dma((n,)),
            dma((n,)),
            dma((pairs, n)),
            dma((2 * n,)),
            dma((3,)),
        ],
        compiler_params=pltpu.CompilerParams(
            collective_id=0, has_side_effects=True, vmem_limit_bytes=60 * 1024 * 1024
        ),
    )(packed.reshape(3, nx * steps // 8, 8, nx), velocity, filter_inverse, block, bins)
    home = home.reshape(n, 6 * pairs * 8, nx)
    leonard, viscosity, coefficient = pl.pallas_call(
        functools.partial(finish_kernel, dims, 2 * nx * nz),
        out_shape=(f32((6, lp, nz, nx)), f32((lp, nz, nx)), f32((1, ny))),
        in_specs=[smem] + [vmem] * 4,
        out_specs=(vmem,) * 3,
    )(chip, home, sums, magnitude, bins)
    return (leonard, viscosity, coefficient.reshape(ny))


def by_blocks(velocity, filter_inverse, filter_block, plane_bin):
    _, lp, nz, nx = velocity.shape
    n = lax.axis_size("pz")
    m = lax.axis_size("px")
    ny, zs = n * lp, nz // n
    win = zs + 4

    same = (filter_block[:, None] == filter_block[None, :]).astype(jnp.float32)
    masked = filter_inverse * same
    weights = masked / jnp.sum(masked, axis=1, keepdims=True)
    onehot = (plane_bin[:, None] == jnp.arange(nx, dtype=jnp.int32)[None, :]).astype(jnp.float32)

    right = lax.ppermute(velocity, "px", [((i + 1) % m, i) for i in range(m)])
    left = right if m == 2 else lax.ppermute(velocity, "px", [(i, (i + 1) % m) for i in range(m)])
    below = lax.ppermute(velocity[:, -1:], "pz", [(i, i + 1) for i in range(n - 1)])
    above = lax.ppermute(velocity[:, :1], "pz", [(i + 1, i) for i in range(n - 1)])
    magnitude = pl.pallas_call(
        magnitude_kernel,
        out_shape=jax.ShapeDtypeStruct((lp, nz, nx), jnp.float32),
        cost_estimate=pl.CostEstimate(flops=60 * lp * nz * nx, bytes_accessed=40 * lp * nz * nx, transcendentals=0),
    )(velocity, right, left, below, above)
    turned = jnp.transpose(velocity, (0, 2, 1, 3))
    turned = jnp.concatenate([turned[:, -2:], turned, turned[:, :2]], axis=1)
    sent = jnp.stack([turned[:, t * zs : t * zs + win] for t in range(n)])
    own = lax.all_to_all(sent, "pz", split_axis=0, concat_axis=0, tiled=True)
    ahead = lax.ppermute(own, "px", [((i + 1) % m, i) for i in range(m)])
    behind = lax.ppermute(own, "px", [(i, (i + 1) % m) for i in range(m)])
    blocks = (own, ahead, behind)

    rows = 6 * zs * lp
    back = pl.pallas_call(
        functools.partial(column_kernel, (n, win, lp, nx), fill_from_blocks, len(blocks)),
        out_shape=jax.ShapeDtypeStruct((n, rows + 8, nx), jnp.float32),
        in_specs=[pl.BlockSpec(memory_space=pltpu.VMEM)] * 5,
        out_specs=pl.BlockSpec(memory_space=pltpu.VMEM),
        scratch_shapes=[
            pltpu.VMEM((3, win, ny + 16, 2 * nx), jnp.float32),
            pltpu.VMEM((21, ny, zs * nx), jnp.bfloat16),
            pltpu.VMEM((21, ny, zs * nx), jnp.bfloat16),
            pltpu.VMEM((21, ny, zs * nx), jnp.float32),
            pltpu.VMEM((ny, nx), jnp.float32),
            pltpu.VMEM((ny, nx), jnp.float32),
            pltpu.VMEM((ny, ny), jnp.bfloat16),
            pltpu.VMEM((ny, ny), jnp.bfloat16),
        ],
        compiler_params=pltpu.CompilerParams(vmem_limit_bytes=60 * 1024 * 1024),
    )(*blocks, weights, onehot)

    home = lax.all_to_all(back, "pz", split_axis=0, concat_axis=0, tiled=True)
    totals = lax.psum(jnp.sum(home[:, rows:], axis=0), "px")
    stress = home[:, :rows].reshape(n, 6, zs, lp, nx)
    leonard = jnp.transpose(stress, (1, 3, 0, 2, 4)).reshape(6, lp, nz, nx)
    numer, denom = totals[0, :NBIN], totals[4, :NBIN]
    cells = nx * m * nz
    per_bin = numer / jnp.maximum(denom, jnp.float32(cells))
    coefficient = jnp.dot(onehot[:, :NBIN], per_bin, precision=lax.Precision.HIGHEST)
    local_coef = lax.dynamic_slice_in_dim(coefficient, lax.axis_index("pz") * lp, lp, 0)
    viscosity = local_coef[:, None, None] * magnitude
    return (leonard, viscosity, coefficient)


def local(*arrays):
    _, lp, nz, nx = arrays[0].shape
    n, m = lax.axis_size("pz"), lax.axis_size("px")
    groups = nx // nz
    fits = m == 2 and n % 2 == 0 and 8 * n == nx and groups * nz == nx and lp == 16 and groups == 4
    if fits:
        return by_strips(*arrays, n)
    return by_blocks(*arrays)


def solution(mesh):
    return jax.shard_map(
        local,
        mesh=mesh,
        in_specs=(P(None, "pz", None, "px"), P(), P(), P()),
        out_specs=(P(None, "pz", None, "px"), P("pz", None, "px"), P()),
        check_vma=False,
    )
```

```python
import functools

import jax
import jax.numpy as jnp
from jax import lax
from jax.experimental import pallas as pl
from jax.experimental.pallas import tpu as pltpu
from jax.sharding import PartitionSpec as P

NBIN = 64
MESH = pl.DeviceIdType.MESH
PAIRS = ((0, 0), (1, 1), (2, 2), (0, 1), (0, 2), (1, 2))


def tensor_norm(s):
    diag = s[0] * s[0] + s[1] * s[1] + s[2] * s[2]
    off = s[3] * s[3] + s[4] * s[4] + s[5] * s[5]
    return jnp.sqrt(2.0 * diag + 4.0 * off)


def strain_of(dx, dy, dz):
    return [
        dx[0] * 0.5,
        dy[1] * 0.5,
        dz[2] * 0.5,
        0.25 * (dy[0] + dx[1]),
        0.25 * (dz[0] + dx[2]),
        0.25 * (dz[1] + dy[2]),
    ]


def fill_from_blocks(dims, ext, own, right, left):
    n, win, lp, nx = dims
    lane = lax.broadcasted_iota(jnp.int32, (lp, nx), 1)
    from_right = lane < nx // 2

    @pl.loop(0, n)
    def _(p):
        rows = pl.ds(pl.multiple_of(8 + p * lp, 8), lp)
        for c in range(3):
            for z in range(win):
                ext[c, z, rows, 0:nx] = own[p, c, z]
                ext[c, z, rows, nx : 2 * nx] = jnp.where(from_right, right[p, c, z], left[p, c, z])


def column_kernel(dims, fill, sources, *refs):
    n, win, lp, nx = dims
    blocks, refs = refs[:sources], refs[sources:]
    weights, onehot, back, ext, bhi, blo, filt, lms, mms, whi, wlo = refs
    zs = win - 4
    ny = n * lp
    lanes = 2 * nx
    heavy = weights[...].astype(jnp.bfloat16)
    whi[...] = heavy
    wlo[...] = (weights[...] - heavy.astype(jnp.float32)).astype(jnp.bfloat16)

    zero = jnp.zeros((8, lanes), jnp.float32)
    for c in range(3):
        for z in range(win):
            ext[c, z, 0:8, :] = zero
            ext[c, z, ny + 8 : ny + 16, :] = zero
    fill(dims, ext, *blocks)

    @pl.loop(0, n)
    def _(p):
        base = pl.multiple_of(p * lp, 8)
        u = [[ext[c, z, pl.ds(base + 8, lp), :] for z in range(win)] for c in range(3)]
        boxes = [[None] * 21 for _ in range(zs)]
        for z in range(1, win - 1):
            v = [u[c][z] for c in range(3)]
            dx, dy, dz = [], [], []
            for c in range(3):
                dx.append(pltpu.roll(v[c], lanes - 1, 1) - pltpu.roll(v[c], 1, 1))
                tall = ext[c, z, pl.ds(base, lp + 16), :]
                dy.append(tall[9 : 9 + lp] - tall[7 : 7 + lp])
                dz.append(u[c][z + 1] - u[c][z - 1])
            s = strain_of(dx, dy, dz)
            mag = tensor_norm(s)
            fields = v + s + [v[i] * v[j] for i, j in PAIRS] + [mag * t for t in s]
            for o in range(zs):
                step = z - (o + 2)
                if -1 <= step <= 1:
                    for k in range(21):
                        term = fields[k] if step else 2.0 * fields[k]
                        boxes[o][k] = term if boxes[o][k] is None else boxes[o][k] + term
        for o in range(zs):
            for k in range(21):
                f = boxes[o][k]
                box = (pltpu.roll(f, 1, 1) + pltpu.roll(f, lanes - 1, 1) + 2.0 * f)[:, :nx] * 0.0625
                high = box.astype(jnp.bfloat16)
                cols = slice(o * nx, (o + 1) * nx)
                bhi[k, pl.ds(base, lp), cols] = high
                blo[k, pl.ds(base, lp), cols] = (box - high.astype(jnp.float32)).astype(jnp.bfloat16)

    @pl.loop(0, 21)
    def _(k):
        dot = functools.partial(jnp.dot, preferred_element_type=jnp.float32)
        filt[k] = dot(whi[...], bhi[k]) + (dot(whi[...], blo[k]) + dot(wlo[...], bhi[k]))

    @pl.loop(0, n)
    def _(p):
        base = pl.multiple_of(p * lp, 8)
        lm_total = jnp.zeros((lp, nx), jnp.float32)
        mm_total = jnp.zeros((lp, nx), jnp.float32)
        for o in range(zs):
            g = [filt[k, pl.ds(base, lp), o * nx : (o + 1) * nx] for k in range(21)]
            fmag = 4.0 * tensor_norm(g[3:9])
            for q, (i, j) in enumerate(PAIRS):
                leonard = g[9 + q] - g[i] * g[j]
                model = g[15 + q] - fmag * g[3 + q]
                weighted = model if q < 3 else 2.0 * model
                lm_total += leonard * weighted
                mm_total += model * weighted
                back[p, (q * zs + o) * lp : (q * zs + o + 1) * lp, :] = leonard
        lms[pl.ds(base, lp), :] = lm_total
        mms[pl.ds(base, lp), :] = mm_total

    ones = jnp.ones((8, nx), jnp.float32)
    exact = functools.partial(
        lax.dot_general, preferred_element_type=jnp.float32, precision=lax.Precision.HIGHEST
    )
    totals = []
    for part in (lms, mms):
        planes = exact(ones, part[...], (((1,), (1,)), ((), ())))
        totals.append(exact(planes, onehot[...], (((1,), (0,)), ((), ()))))
    row = lax.broadcasted_iota(jnp.int32, (8, onehot.shape[1]), 0)
    tile = jnp.where(row < 4, totals[0], totals[1])
    for p in range(n):
        back[p, 6 * zs * lp :, :] = tile


def greet_all(m, n):
    me = lax.axis_index("px") * n + lax.axis_index("pz")
    barrier = pltpu.get_barrier_semaphore()

    @pl.loop(1, m * n)
    def _(step):
        peer = lax.rem(me + step, m * n)
        pl.semaphore_signal(barrier, inc=1, device_id=(peer // n, lax.rem(peer, n)), device_id_type=MESH)

    pl.semaphore_wait(barrier, m * n - 1)


def magnitude_kernel(centre, right, left, below, above, out):
    _, lp, nz, nx = centre.shape
    lane = lax.broadcasted_iota(jnp.int32, (nz, nx), 1)
    for y in range(lp):
        v = [centre[c, y] for c in range(3)]
        dx, dy, dz = [], [], []
        for c in range(3):
            ahead = jnp.where(lane == nx - 1, pltpu.roll(right[c, y], nx - 1, 1), pltpu.roll(v[c], nx - 1, 1))
            behind = jnp.where(lane == 0, pltpu.roll(left[c, y], 1, 1), pltpu.roll(v[c], 1, 1))
            dx.append(ahead - behind)
            dz.append(pltpu.roll(v[c], nz - 1, 0) - pltpu.roll(v[c], 1, 0))
            up = centre[c, y + 1] if y + 1 < lp else above[c, 0]
            down = centre[c, y - 1] if y else below[c, 0]
            dy.append(up - down)
        out[y] = tensor_norm(strain_of(dx, dy, dz))


def swap_bit(first, second, bit):
    nx = first.shape[-1]
    low = (lax.broadcasted_iota(jnp.int32, first.shape, 1) & bit) == 0
    return (
        jnp.where(low, first, pltpu.roll(second, bit, 1)),
        jnp.where(low, pltpu.roll(first, nx - bit, 1), second),
    )


def pack_kernel(dims, velocity, packed):
    lp, nz, nx = dims
    groups = nx // nz
    steps = lp // groups

    @pl.loop(0, 3)
    def _(c):
        for q in range(steps):
            rows = jnp.concatenate([velocity[c, g * steps + q] for g in range(groups)], axis=0)
            packed[c, pl.ds(q, nx, stride=steps), :] = rows.T


def plane_order(shape, lp, nx, dim):
    at = lax.broadcasted_iota(jnp.int32, shape, dim)
    return (at % nx) // 8 * lp + at // nx * 8 + at % 8


def column_weights(dims, upper, inverse, block, bins, wide, heavy, onehot):
    ny, lp, nx = dims
    rows = ny // 2
    label = jnp.broadcast_to(block[...].astype(jnp.float32), (ny, ny))
    turned = label.T
    mine = jnp.where(upper, turned[rows:], turned[:rows])
    masked = jnp.where(label[:rows] == mine, jnp.where(upper, inverse[rows:, :], inverse[:rows, :]), 0.0)
    weights = masked / jnp.sum(masked, axis=1, keepdims=True) * 0.0625
    order = plane_order((ny, ny), lp, nx, 0) == lax.broadcasted_iota(jnp.int32, (ny, ny), 1)
    order = order.astype(jnp.float32).astype(jnp.bfloat16)

    def placed(part):
        dims = (((1,), (1,)), ((), ()))
        return lax.dot_general(order, part, dims, preferred_element_type=jnp.float32).astype(jnp.bfloat16)

    head = weights.astype(jnp.bfloat16)
    rest = (weights - head.astype(jnp.float32)).astype(jnp.bfloat16)
    heavy[...] = placed(head)
    wide[:, :rows] = heavy[...]
    wide[:, rows:] = placed(rest)
    label = jnp.where(upper, bins[:, rows:], bins[:, :rows])
    kind = lax.broadcasted_iota(jnp.int32, (nx, rows), 0)
    onehot[...] = (jnp.broadcast_to(label, (nx, rows)) == kind).astype(jnp.float32)


def flip_bits(value, mask, count):
    out = 0
    for bit in range(count):
        digit = lax.rem(value // (1 << bit), 2)
        out = out + (1 << bit) * ((1 - digit) if mask >> bit & 1 else digit)
    return out


def plane_magnitudes(velocity, beside, near, out, has_below, has_above):
    _, lp, nz, nx = velocity.shape
    lane = lax.broadcasted_iota(jnp.int32, (nz, nx), 1)

    def plane(y, ups, downs):
        dx, dy, dz = [], [], []
        for c in range(3):
            v, side = velocity[c, y], beside[c, y]
            ahead = jnp.where(lane == nx - 1, pltpu.roll(side, nx - 1, 1), pltpu.roll(v, nx - 1, 1))
            behind = jnp.where(lane == 0, pltpu.roll(side, 1, 1), pltpu.roll(v, 1, 1))
            dx.append(ahead - behind)
            dz.append(pltpu.roll(v, nz - 1, 0) - pltpu.roll(v, 1, 0))
            dy.append(ups[c] - downs[c])
        out[y] = tensor_norm(strain_of(dx, dy, dz))

    line = [near[0, c] * has_below for c in range(3)]
    plane(0, [velocity[c, 1] for c in range(3)], line)
    line = [near[1, c] * has_above for c in range(3)]
    plane(lp - 1, line, [velocity[c, lp - 2] for c in range(3)])

    @pl.loop(1, lp - 1)
    def _(y):
        plane(y, [velocity[c, y + 1] for c in range(3)], [velocity[c, y - 1] for c in range(3)])


def unpack_pair(held, u, slot, nz, nx):
    for c in range(3):
        turned = held[:, c, slot].reshape(nx, nx).T
        for hf in range(2):
            first = turned[2 * hf * nz : (2 * hf + 1) * nz]
            second = turned[(2 * hf + 1) * nz : (2 * hf + 2) * nz]
            u[c, hf, 2 * slot], u[c, hf, 2 * slot + 1] = swap_bit(first, second, 4)


def field_columns(u, fields, start, count, nz, nx):
    lane = lax.broadcasted_iota(jnp.int32, (nz, nx), 1)
    last, first_lane = lane % 8 == 7, lane % 8 == 0
    top, bottom = lane == nx - 1, lane == 0

    @pl.loop(0, count, unroll=2)
    def _(i):
        x = start + i
        here, dx, dy, dz = [], [], [], []
        for c in range(3):
            v = [u[c, hf, x] for hf in range(2)]
            here.append(v)
            dx.append([u[c, hf, x + 1] - u[c, hf, x - 1] for hf in range(2)])
            dz.append([pltpu.roll(v[hf], nz - 1, 0) - pltpu.roll(v[hf], 1, 0) for hf in range(2)])
            ahead = [pltpu.roll(v[hf], nx - 1, 1) for hf in range(2)]
            behind = [pltpu.roll(v[hf], 1, 1) for hf in range(2)]
            up = [
                jnp.where(last, pltpu.roll(v[1], 7, 1), ahead[0]),
                jnp.where(last, jnp.where(top, 0.0, ahead[0]), ahead[1]),
            ]
            down = [
                jnp.where(first_lane, jnp.where(bottom, 0.0, behind[1]), behind[0]),
                jnp.where(first_lane, pltpu.roll(v[0], nx - 7, 1), behind[1]),
            ]
            dy.append([up[hf] - down[hf] for hf in range(2)])
        for hf in range(2):
            gx, gy, gz = [d[hf] for d in dx], [d[hf] for d in dy], [d[hf] for d in dz]
            s = [gx[0] + gx[0], gy[1] + gy[1], gz[2] + gz[2], gy[0] + gx[1], gz[0] + gx[2], gz[1] + gy[2]]
            mag = tensor_norm(s)
            for c in range(3):
                fields[c, x, hf] = here[c][hf]
            for q, (i, j) in enumerate(PAIRS):
                fields[3 + q, x, hf] = s[q]
                fields[9 + q, x, hf] = here[i][hf] * here[j][hf]
                fields[15 + q, x, hf] = mag * s[q]


def filter_pair(fields, start, high, low, filt, wide, heavy, nz):
    cells = 2 * nz

    rows = wide.shape[1] // 2

    def box(k):
        columns = []
        for hf in range(2):
            f = [fields[k, start + i, hf] for i in range(4)]
            pair = [f[i] + f[i + 1] for i in range(3)]
            parts = []
            for i in range(2):
                along = pair[i] + pair[i + 1]
                parts.append(pltpu.roll(along, 1, 0) + pltpu.roll(along, nz - 1, 0) + (along + along))
            columns.append(jnp.concatenate(parts, axis=0))
        whole = jnp.concatenate(columns, axis=1)
        head = whole.astype(jnp.bfloat16)
        high[k * cells : (k + 1) * cells, :] = head
        low[k * cells : (k + 1) * cells, :] = (whole - head.astype(jnp.float32)).astype(jnp.bfloat16)

    dot = functools.partial(jnp.dot, preferred_element_type=jnp.float32)
    for b in range(4):
        if b < 3:
            for k in range(7 * b, 7 * b + 7):
                box(k)
        if b:
            at = slice((b - 1) * 7 * cells, b * 7 * cells)
            both = dot(high[at, :], wide[...])
            filt[at, :] = both[:, :rows] + (dot(low[at, :], heavy[...]) + both[:, rows:])


def stress_pair(filt, stress, sums, place, nz):
    cells = 2 * nz

    @pl.loop(0, cells // 8)
    def _(r):
        base = pl.multiple_of(8 * r, 8)
        g = [filt[pl.ds(base + k * cells, 8), :] for k in range(21)]
        fmag = 4.0 * tensor_norm(g[3:9])
        lm_total, mm_total = None, None
        at = pl.ds(pl.multiple_of(place * cells + base, 8), 8)
        for q, (i, j) in enumerate(PAIRS):
            leonard = g[9 + q] - g[i] * g[j]
            model = g[15 + q] - fmag * g[3 + q]
            weighted = model if q < 3 else 2.0 * model
            lm_total = leonard * weighted if q == 0 else lm_total + leonard * weighted
            mm_total = model * weighted if q == 0 else mm_total + model * weighted
            stress[q, at, :] = leonard
        sums[0] += lm_total
        sums[1] += mm_total


def flow_kernel(
    dims, packed, velocity, inverse, block, bins, home, totals, magnitude,
    held, u, fields, high, low, filt, stress, back, wide, heavy, onehot, sums, tile, beside, near,
    main_out, edge_out, pass_out, back_out, sum_out, halo_out,
    main_in, edge_in, pass_in, back_in, sum_in, halo_in,
):
    n, pairs, lp, nz, nx = dims
    ny, h = n * lp, n // 2
    strips = h // 2
    whole = 2 * pairs
    a, s = lax.axis_index("px"), lax.axis_index("pz")
    half, spot = s // h, lax.rem(s, h)
    remote = functools.partial(pltpu.make_async_remote_copy, device_id_type=MESH)
    greet_all(2, n)

    def send(source, dst, core, chip, out_sem, in_sem):
        itself = (core == a) & (chip == s)
        copy = remote(source, dst, out_sem, in_sem, device_id=(core, chip))
        return itself, copy, pltpu.make_async_copy(source, dst, in_sem)

    def start(moves):
        for itself, copy, here in moves:
            pl.when(itself)(here.start)
            pl.when(jnp.logical_not(itself))(copy.start)

    def drain(moves):
        for itself, copy, here in moves:
            pl.when(jnp.logical_not(itself))(copy.wait_send)

    def edges(r):
        t, i = r // strips, lax.rem(r, strips)
        strip = strips * a + i
        left = packed.at[:, pl.ds(whole * i + whole - 1, 1)]
        yield send(left, held.at[s, :, 0:1], 0, h * t + lax.rem(strip + 1, h), edge_out.at[0, r], edge_in.at[s])
        right = packed.at[:, pl.ds(whole * i, 1)]
        yield send(right, held.at[s, :, pairs + 1 : pairs + 2], 1, h * t + lax.rem(strip + h - 1, h), edge_out.at[1, r], edge_in.at[s])

    def mains(r, m):
        t, i = r // strips, lax.rem(r, strips)
        for core in range(2):
            own = m if core else pairs - 1 - m
            source = packed.at[:, pl.ds(whole * i + pairs * core + own, 1)]
            dst = held.at[s, :, pl.ds(own + 1, 1)]
            yield send(source, dst, core, h * t + strips * a + i, main_out.at[m, core, r], main_in.at[m, s])

    def ordered(r):
        return lax.rem(half + 1 + r // strips, 2) * strips + lax.rem(s + r, strips)

    halos = [
        remote(velocity, beside, halo_out.at[0], halo_in.at[0], device_id=(1 - a, s)),
        remote(velocity.at[:, lp - 1], near.at[0], halo_out.at[1], halo_in.at[1], device_id=(a, lax.rem(s + 1, n))),
        remote(velocity.at[:, 0], near.at[1], halo_out.at[2], halo_in.at[2], device_id=(a, lax.rem(s + n - 1, n))),
    ]
    for copy in halos:
        copy.start()

    @pl.loop(0, pairs)
    def _(m):
        @pl.loop(0, h)
        def _(r):
            start(mains(ordered(r), m))

    @pl.loop(0, h)
    def _(r):
        start(edges(ordered(r)))

    column_weights((ny, lp, nx), half == 1, inverse, block, bins, wide, heavy, onehot)
    sums[...] = jnp.zeros(sums.shape, jnp.float32)

    def slot_of(m):
        return pairs - m + a * (1 + 2 * m - pairs)

    def forward(p):
        return remote(
            held.at[p, :, pl.ds(slot_of(0), 1)], held.at[p, :, pl.ds((pairs + 1) * a, 1)],
            pass_out.at[p], pass_in.at[p], device_id=(1 - a, s),
        )

    def await_pair(sem, p):
        pltpu.make_async_copy(packed.at[:, 0:1], held.at[p, :, 0:1], sem).wait()

    mine = 2 * lax.rem(spot, strips) + a

    def returns(j, d):
        place = pairs // 2 - 1 - j + a * (1 + 2 * j - pairs // 2)
        source, dst = back.at[j, d], home.at[mine, :, place]
        return [send(source, dst, spot // strips, h * half + d, back_out.at[j, d], back_in.at[j, mine])]

    def column(m, count):
        q = slot_of(m)
        field_columns(u, fields, 2 * q - 1 if count == 4 else 2 * q - 1 + 2 * a, count, nz, nx)
        filter_pair(fields, 2 * q - 1, high, low, filt, wide, heavy, nz)
        stress_pair(filt, stress, sums, lax.rem(q - 1, 2), nz)

    def give_back(j):
        @pl.loop(0, 6)
        def _(f):
            rows = [stress[f, x * nz : (x + 1) * nz, :] for x in range(4)]
            rows[0], rows[1] = swap_bit(rows[0], rows[1], 4)
            rows[2], rows[3] = swap_bit(rows[2], rows[3], 4)
            rows[0], rows[2] = swap_bit(rows[0], rows[2], 8)
            rows[1], rows[3] = swap_bit(rows[1], rows[3], 8)
            back[j, :, f] = jnp.concatenate(rows, axis=0).T.reshape(h, lp, nx)

        for r in range(h):
            start(returns(j, flip_bits(spot, h - 1 - r, h.bit_length() - 1)))

    for copy in halos:
        copy.wait()
    plane_magnitudes(velocity, beside, near, magnitude, (s > 0).astype(jnp.float32), (s < n - 1).astype(jnp.float32))

    @pl.loop(0, n)
    def _(p):
        await_pair(main_in.at[0, p], p)
        forward(p).start()

    unpack_pair(held, u, slot_of(0), nz, nx)

    @pl.loop(0, n)
    def _(p):
        forward(p).wait()
        await_pair(main_in.at[1, p], p)

    unpack_pair(held, u, slot_of(-1), nz, nx)
    unpack_pair(held, u, slot_of(1), nz, nx)
    column(0, 4)

    @pl.loop(1, pairs)
    def _(m):
        @pl.when(m < pairs - 1)
        def _():
            @pl.loop(0, n)
            def _(p):
                await_pair(main_in.at[m + 1, p], p)

        @pl.when(m == pairs - 1)
        def _():
            @pl.loop(0, n)
            def _(p):
                await_pair(edge_in.at[p], p)

        unpack_pair(held, u, slot_of(m + 1), nz, nx)
        column(m, 2)

        @pl.when(lax.rem(m, 2) == 1)
        def _():
            give_back(m // 2)

    exact = functools.partial(
        lax.dot_general, dimension_numbers=(((1,), (1,)), ((), ())),
        preferred_element_type=jnp.float32, precision=lax.Precision.HIGHEST,
    )
    lm_bins = jnp.sum(exact(sums[0], onehot[...]), axis=0, keepdims=True) * (1.0 / 16.0)
    mm_bins = jnp.sum(exact(sums[1], onehot[...]), axis=0, keepdims=True) * (1.0 / 256.0)
    row = lax.broadcasted_iota(jnp.int32, (8, nx), 0)
    tile[...] = jnp.where(row < 4, lm_bins, mm_bins)
    me = a * n + s

    def share(t):
        return [send(tile, totals.at[me], t // n, lax.rem(t, n), sum_out.at[t], sum_in.at[me])]

    @pl.loop(0, 2 * n)
    def _(r):
        start(share(lax.rem(me + r, 2 * n)))

    @pl.loop(0, h)
    def _(r):
        drain(edges(r))

        @pl.loop(0, pairs)
        def _(m):
            drain(mains(r, m))

    @pl.loop(0, h)
    def _(p):
        for j in range(pairs // 2):
            pltpu.make_async_copy(back.at[0, 0], home.at[p, :, 0], back_in.at[j, p]).wait()
            drain(returns(j, p))

    @pl.loop(0, 2 * n)
    def _(t):
        pltpu.make_async_copy(tile, totals.at[t], sum_in.at[t]).wait()
        drain(share(t))


def finish_kernel(dims, cells, chip, home, sums, magnitude, bins, leonard, viscosity, coefficient):
    n, pairs, lp, nz, nx = dims
    ny, groups = n * lp, nx // nz
    steps = lp // groups
    total = sums[0]
    for p in range(1, 2 * n):
        total = total + sums[p]
    numer, denom = total[0:1, :], total[4:5, :]
    per_bin = numer / jnp.maximum(denom, jnp.float32(cells))
    exact = functools.partial(
        lax.dot_general, preferred_element_type=jnp.float32, precision=lax.Precision.HIGHEST
    )
    label = jnp.broadcast_to(bins[...].astype(jnp.float32), (nx, ny))
    kind = lax.broadcasted_iota(jnp.int32, (nx, ny), 0).astype(jnp.float32)
    onehot = (label == kind).astype(jnp.float32)
    table = jnp.broadcast_to(per_bin, (nx, nx))
    coefficient[...] = exact(table[0:8], onehot, (((1,), (0,)), ((), ())))[0:1, :]
    mine = jnp.zeros((nx, lp), jnp.float32)
    for s in range(n):
        mine = jnp.where(chip[0] == s, onehot[:, s * lp : (s + 1) * lp], mine)
    spread = exact(mine, table, (((0,), (1,)), ((), ())))
    for y in range(lp):
        viscosity[y] = spread[y : y + 1, :] * magnitude[y]

    @pl.loop(0, 6)
    def _(f):
        for q in range(steps):
            at = pl.ds(f * pairs * 8 + q, 2 * pairs, stride=steps)
            turned = jnp.concatenate([home[p, at, :] for p in range(nx // (2 * pairs))], axis=0).T
            for g in range(groups):
                leonard[f, g * steps + q] = turned[g * nz : (g + 1) * nz]


def by_strips(velocity, filter_inverse, filter_block, plane_bin, n):
    _, lp, nz, nx = velocity.shape
    ny, h = n * lp, n // 2
    pairs = nx // h // 2
    dims = (n, pairs, lp, nz, nx)
    steps = lp // (nx // nz)
    chip = lax.axis_index("pz").astype(jnp.int32).reshape(1)
    block = filter_block.reshape(1, ny)
    bins = plane_bin.reshape(1, ny)
    vmem = pl.BlockSpec(memory_space=pltpu.VMEM)
    smem = pl.BlockSpec(memory_space=pltpu.SMEM)
    f32 = functools.partial(jax.ShapeDtypeStruct, dtype=jnp.float32)
    dma = pltpu.SemaphoreType.DMA

    packed = pl.pallas_call(
        functools.partial(pack_kernel, (lp, nz, nx)),
        out_shape=f32((3, nx * steps, nx)),
        in_specs=[vmem],
        out_specs=vmem,
    )(velocity)
    room = functools.partial(pltpu.VMEM, dtype=jnp.float32)
    home, sums, magnitude = pl.pallas_call(
        functools.partial(flow_kernel, dims),
        out_shape=(f32((h, 6, pairs // 2, lp, nx)), f32((2 * n, 8, nx)), f32((lp, nz, nx))),
        in_specs=[vmem] * 5,
        out_specs=(vmem,) * 3,
        scratch_shapes=[
            room((n, 3, pairs + 2, 8, nx)),
            room((3, 2, 2 * pairs + 4, nz, nx)),
            room((21, 2 * pairs + 4, 2, nz, nx)),
            pltpu.VMEM((21 * 2 * nz, ny), jnp.bfloat16),
            pltpu.VMEM((21 * 2 * nz, ny), jnp.bfloat16),
            room((21 * 2 * nz, ny // 2)),
            room((6, 4 * nz, nx)),
            room((pairs // 2, h, 6, lp, nx)),
            pltpu.VMEM((ny, ny), jnp.bfloat16),
            pltpu.VMEM((ny, ny // 2), jnp.bfloat16),
            room((nx, ny // 2)),
            room((2, 8, ny // 2)),
            room((8, nx)),
            room((3, lp, nz, nx)),
            room((2, 3, nz, nx)),
            dma((pairs, 2, h)),
            dma((2, h)),
            dma((n,)),
            dma((pairs // 2, h)),
            dma((2 * n,)),
            dma((3,)),
            dma((pairs, n)),
            dma((n,)),
            dma((n,)),
            dma((pairs // 2, h)),
            dma((2 * n,)),
            dma((3,)),
        ],
        compiler_params=pltpu.CompilerParams(
            collective_id=0, has_side_effects=True, vmem_limit_bytes=60 * 1024 * 1024
        ),
    )(packed.reshape(3, nx * steps // 8, 8, nx), velocity, filter_inverse, block, bins)
    home = home.reshape(h, 6 * pairs // 2 * lp, nx)
    leonard, viscosity, coefficient = pl.pallas_call(
        functools.partial(finish_kernel, dims, 2 * nx * nz),
        out_shape=(f32((6, lp, nz, nx)), f32((lp, nz, nx)), f32((1, ny))),
        in_specs=[smem] + [vmem] * 4,
        out_specs=(vmem,) * 3,
    )(chip, home, sums, magnitude, bins)
    return (leonard, viscosity, coefficient.reshape(ny))


def by_blocks(velocity, filter_inverse, filter_block, plane_bin):
    _, lp, nz, nx = velocity.shape
    n = lax.axis_size("pz")
    m = lax.axis_size("px")
    ny, zs = n * lp, nz // n
    win = zs + 4

    same = (filter_block[:, None] == filter_block[None, :]).astype(jnp.float32)
    masked = filter_inverse * same
    weights = masked / jnp.sum(masked, axis=1, keepdims=True)
    onehot = (plane_bin[:, None] == jnp.arange(nx, dtype=jnp.int32)[None, :]).astype(jnp.float32)

    right = lax.ppermute(velocity, "px", [((i + 1) % m, i) for i in range(m)])
    left = right if m == 2 else lax.ppermute(velocity, "px", [(i, (i + 1) % m) for i in range(m)])
    below = lax.ppermute(velocity[:, -1:], "pz", [(i, i + 1) for i in range(n - 1)])
    above = lax.ppermute(velocity[:, :1], "pz", [(i + 1, i) for i in range(n - 1)])
    magnitude = pl.pallas_call(
        magnitude_kernel,
        out_shape=jax.ShapeDtypeStruct((lp, nz, nx), jnp.float32),
        cost_estimate=pl.CostEstimate(flops=60 * lp * nz * nx, bytes_accessed=40 * lp * nz * nx, transcendentals=0),
    )(velocity, right, left, below, above)
    turned = jnp.transpose(velocity, (0, 2, 1, 3))
    turned = jnp.concatenate([turned[:, -2:], turned, turned[:, :2]], axis=1)
    sent = jnp.stack([turned[:, t * zs : t * zs + win] for t in range(n)])
    own = lax.all_to_all(sent, "pz", split_axis=0, concat_axis=0, tiled=True)
    ahead = lax.ppermute(own, "px", [((i + 1) % m, i) for i in range(m)])
    behind = lax.ppermute(own, "px", [(i, (i + 1) % m) for i in range(m)])
    blocks = (own, ahead, behind)

    rows = 6 * zs * lp
    back = pl.pallas_call(
        functools.partial(column_kernel, (n, win, lp, nx), fill_from_blocks, len(blocks)),
        out_shape=jax.ShapeDtypeStruct((n, rows + 8, nx), jnp.float32),
        in_specs=[pl.BlockSpec(memory_space=pltpu.VMEM)] * 5,
        out_specs=pl.BlockSpec(memory_space=pltpu.VMEM),
        scratch_shapes=[
            pltpu.VMEM((3, win, ny + 16, 2 * nx), jnp.float32),
            pltpu.VMEM((21, ny, zs * nx), jnp.bfloat16),
            pltpu.VMEM((21, ny, zs * nx), jnp.bfloat16),
            pltpu.VMEM((21, ny, zs * nx), jnp.float32),
            pltpu.VMEM((ny, nx), jnp.float32),
            pltpu.VMEM((ny, nx), jnp.float32),
            pltpu.VMEM((ny, ny), jnp.bfloat16),
            pltpu.VMEM((ny, ny), jnp.bfloat16),
        ],
        compiler_params=pltpu.CompilerParams(vmem_limit_bytes=60 * 1024 * 1024),
    )(*blocks, weights, onehot)

    home = lax.all_to_all(back, "pz", split_axis=0, concat_axis=0, tiled=True)
    totals = lax.psum(jnp.sum(home[:, rows:], axis=0), "px")
    stress = home[:, :rows].reshape(n, 6, zs, lp, nx)
    leonard = jnp.transpose(stress, (1, 3, 0, 2, 4)).reshape(6, lp, nz, nx)
    numer, denom = totals[0, :NBIN], totals[4, :NBIN]
    cells = nx * m * nz
    per_bin = numer / jnp.maximum(denom, jnp.float32(cells))
    coefficient = jnp.dot(onehot[:, :NBIN], per_bin, precision=lax.Precision.HIGHEST)
    local_coef = lax.dynamic_slice_in_dim(coefficient, lax.axis_index("pz") * lp, lp, 0)
    viscosity = local_coef[:, None, None] * magnitude
    return (leonard, viscosity, coefficient)


def local(*arrays):
    _, lp, nz, nx = arrays[0].shape
    n, m = lax.axis_size("pz"), lax.axis_size("px")
    groups = nx // nz
    fits = m == 2 and n % 4 == 0 and 8 * n == nx and groups * nz == nx and lp == 16 and groups == 4
    if fits:
        return by_strips(*arrays, n)
    return by_blocks(*arrays)


def solution(mesh):
    return jax.shard_map(
        local,
        mesh=mesh,
        in_specs=(P(None, "pz", None, "px"), P(), P(), P()),
        out_specs=(P(None, "pz", None, "px"), P("pz", None, "px"), P()),
        check_vma=False,
    )
```

```python
import functools

import jax
import jax.numpy as jnp
from jax import lax
from jax.experimental import pallas as pl
from jax.experimental.pallas import tpu as pltpu
from jax.sharding import PartitionSpec as P

NBIN = 64
MESH = pl.DeviceIdType.MESH
PAIRS = ((0, 0), (1, 1), (2, 2), (0, 1), (0, 2), (1, 2))


def tensor_norm(s):
    diag = s[0] * s[0] + s[1] * s[1] + s[2] * s[2]
    off = s[3] * s[3] + s[4] * s[4] + s[5] * s[5]
    return jnp.sqrt(2.0 * diag + 4.0 * off)


def strain_of(dx, dy, dz):
    return [
        dx[0] * 0.5,
        dy[1] * 0.5,
        dz[2] * 0.5,
        0.25 * (dy[0] + dx[1]),
        0.25 * (dz[0] + dx[2]),
        0.25 * (dz[1] + dy[2]),
    ]


def fill_from_blocks(dims, ext, own, right, left):
    n, win, lp, nx = dims
    lane = lax.broadcasted_iota(jnp.int32, (lp, nx), 1)
    from_right = lane < nx // 2

    @pl.loop(0, n)
    def _(p):
        rows = pl.ds(pl.multiple_of(8 + p * lp, 8), lp)
        for c in range(3):
            for z in range(win):
                ext[c, z, rows, 0:nx] = own[p, c, z]
                ext[c, z, rows, nx : 2 * nx] = jnp.where(from_right, right[p, c, z], left[p, c, z])


def column_kernel(dims, fill, sources, *refs):
    n, win, lp, nx = dims
    blocks, refs = refs[:sources], refs[sources:]
    weights, onehot, back, ext, bhi, blo, filt, lms, mms, whi, wlo = refs
    zs = win - 4
    ny = n * lp
    lanes = 2 * nx
    heavy = weights[...].astype(jnp.bfloat16)
    whi[...] = heavy
    wlo[...] = (weights[...] - heavy.astype(jnp.float32)).astype(jnp.bfloat16)

    zero = jnp.zeros((8, lanes), jnp.float32)
    for c in range(3):
        for z in range(win):
            ext[c, z, 0:8, :] = zero
            ext[c, z, ny + 8 : ny + 16, :] = zero
    fill(dims, ext, *blocks)

    @pl.loop(0, n)
    def _(p):
        base = pl.multiple_of(p * lp, 8)
        u = [[ext[c, z, pl.ds(base + 8, lp), :] for z in range(win)] for c in range(3)]
        boxes = [[None] * 21 for _ in range(zs)]
        for z in range(1, win - 1):
            v = [u[c][z] for c in range(3)]
            dx, dy, dz = [], [], []
            for c in range(3):
                dx.append(pltpu.roll(v[c], lanes - 1, 1) - pltpu.roll(v[c], 1, 1))
                tall = ext[c, z, pl.ds(base, lp + 16), :]
                dy.append(tall[9 : 9 + lp] - tall[7 : 7 + lp])
                dz.append(u[c][z + 1] - u[c][z - 1])
            s = strain_of(dx, dy, dz)
            mag = tensor_norm(s)
            fields = v + s + [v[i] * v[j] for i, j in PAIRS] + [mag * t for t in s]
            for o in range(zs):
                step = z - (o + 2)
                if -1 <= step <= 1:
                    for k in range(21):
                        term = fields[k] if step else 2.0 * fields[k]
                        boxes[o][k] = term if boxes[o][k] is None else boxes[o][k] + term
        for o in range(zs):
            for k in range(21):
                f = boxes[o][k]
                box = (pltpu.roll(f, 1, 1) + pltpu.roll(f, lanes - 1, 1) + 2.0 * f)[:, :nx] * 0.0625
                high = box.astype(jnp.bfloat16)
                cols = slice(o * nx, (o + 1) * nx)
                bhi[k, pl.ds(base, lp), cols] = high
                blo[k, pl.ds(base, lp), cols] = (box - high.astype(jnp.float32)).astype(jnp.bfloat16)

    @pl.loop(0, 21)
    def _(k):
        dot = functools.partial(jnp.dot, preferred_element_type=jnp.float32)
        filt[k] = dot(whi[...], bhi[k]) + (dot(whi[...], blo[k]) + dot(wlo[...], bhi[k]))

    @pl.loop(0, n)
    def _(p):
        base = pl.multiple_of(p * lp, 8)
        lm_total = jnp.zeros((lp, nx), jnp.float32)
        mm_total = jnp.zeros((lp, nx), jnp.float32)
        for o in range(zs):
            g = [filt[k, pl.ds(base, lp), o * nx : (o + 1) * nx] for k in range(21)]
            fmag = 4.0 * tensor_norm(g[3:9])
            for q, (i, j) in enumerate(PAIRS):
                leonard = g[9 + q] - g[i] * g[j]
                model = g[15 + q] - fmag * g[3 + q]
                weighted = model if q < 3 else 2.0 * model
                lm_total += leonard * weighted
                mm_total += model * weighted
                back[p, (q * zs + o) * lp : (q * zs + o + 1) * lp, :] = leonard
        lms[pl.ds(base, lp), :] = lm_total
        mms[pl.ds(base, lp), :] = mm_total

    ones = jnp.ones((8, nx), jnp.float32)
    exact = functools.partial(
        lax.dot_general, preferred_element_type=jnp.float32, precision=lax.Precision.HIGHEST
    )
    totals = []
    for part in (lms, mms):
        planes = exact(ones, part[...], (((1,), (1,)), ((), ())))
        totals.append(exact(planes, onehot[...], (((1,), (0,)), ((), ()))))
    row = lax.broadcasted_iota(jnp.int32, (8, onehot.shape[1]), 0)
    tile = jnp.where(row < 4, totals[0], totals[1])
    for p in range(n):
        back[p, 6 * zs * lp :, :] = tile


def greet_all(m, n):
    me = lax.axis_index("px") * n + lax.axis_index("pz")
    barrier = pltpu.get_barrier_semaphore()

    @pl.loop(1, m * n)
    def _(step):
        peer = lax.rem(me + step, m * n)
        pl.semaphore_signal(barrier, inc=1, device_id=(peer // n, lax.rem(peer, n)), device_id_type=MESH)

    pl.semaphore_wait(barrier, m * n - 1)


def magnitude_kernel(centre, right, left, below, above, out):
    _, lp, nz, nx = centre.shape
    lane = lax.broadcasted_iota(jnp.int32, (nz, nx), 1)
    for y in range(lp):
        v = [centre[c, y] for c in range(3)]
        dx, dy, dz = [], [], []
        for c in range(3):
            ahead = jnp.where(lane == nx - 1, pltpu.roll(right[c, y], nx - 1, 1), pltpu.roll(v[c], nx - 1, 1))
            behind = jnp.where(lane == 0, pltpu.roll(left[c, y], 1, 1), pltpu.roll(v[c], 1, 1))
            dx.append(ahead - behind)
            dz.append(pltpu.roll(v[c], nz - 1, 0) - pltpu.roll(v[c], 1, 0))
            up = centre[c, y + 1] if y + 1 < lp else above[c, 0]
            down = centre[c, y - 1] if y else below[c, 0]
            dy.append(up - down)
        out[y] = tensor_norm(strain_of(dx, dy, dz))


def swap_bit(first, second, bit):
    nx = first.shape[-1]
    low = (lax.broadcasted_iota(jnp.int32, first.shape, 1) & bit) == 0
    return (
        jnp.where(low, first, pltpu.roll(second, bit, 1)),
        jnp.where(low, pltpu.roll(first, nx - bit, 1), second),
    )


def pack_planes(velocity, packed):
    _, lp, nz, nx = velocity.shape
    groups = nx // nz
    steps = lp // groups
    for c in range(3):
        for q in range(steps):
            rows = jnp.concatenate([velocity[c, g * steps + q] for g in range(groups)], axis=0)
            packed[c, pl.ds(q, nx, stride=steps), :] = rows.T


def plane_order(shape, lp, nx, dim):
    at = lax.broadcasted_iota(jnp.int32, shape, dim)
    return (at % nx) // 8 * lp + at // nx * 8 + at % 8


def column_weights(dims, upper, inverse, block, bins, wide, heavy, onehot):
    ny, lp, nx = dims
    rows = ny // 2
    label = jnp.broadcast_to(block[...].astype(jnp.float32), (ny, ny))
    turned = label.T
    mine = jnp.where(upper, turned[rows:], turned[:rows])
    masked = jnp.where(label[:rows] == mine, jnp.where(upper, inverse[rows:, :], inverse[:rows, :]), 0.0)
    weights = masked / jnp.sum(masked, axis=1, keepdims=True) * 0.0625
    order = plane_order((ny, ny), lp, nx, 0) == lax.broadcasted_iota(jnp.int32, (ny, ny), 1)
    order = order.astype(jnp.float32).astype(jnp.bfloat16)

    def placed(part):
        dims = (((1,), (1,)), ((), ()))
        return lax.dot_general(order, part, dims, preferred_element_type=jnp.float32).astype(jnp.bfloat16)

    head = weights.astype(jnp.bfloat16)
    rest = (weights - head.astype(jnp.float32)).astype(jnp.bfloat16)
    heavy[...] = placed(head)
    wide[:, :rows] = heavy[...]
    wide[:, rows:] = placed(rest)
    label = jnp.where(upper, bins[:, rows:], bins[:, :rows])
    kind = lax.broadcasted_iota(jnp.int32, (nx, rows), 0)
    onehot[...] = (jnp.broadcast_to(label, (nx, rows)) == kind).astype(jnp.float32)


def flip_bits(value, mask, count):
    out = 0
    for bit in range(count):
        digit = lax.rem(value // (1 << bit), 2)
        out = out + (1 << bit) * ((1 - digit) if mask >> bit & 1 else digit)
    return out


def plane_magnitudes(velocity, beside, near, out, has_below, has_above):
    _, lp, nz, nx = velocity.shape
    lane = lax.broadcasted_iota(jnp.int32, (nz, nx), 1)

    def plane(y, ups, downs):
        dx, dy, dz = [], [], []
        for c in range(3):
            v, side = velocity[c, y], beside[c, y]
            ahead = jnp.where(lane == nx - 1, pltpu.roll(side, nx - 1, 1), pltpu.roll(v, nx - 1, 1))
            behind = jnp.where(lane == 0, pltpu.roll(side, 1, 1), pltpu.roll(v, 1, 1))
            dx.append(ahead - behind)
            dz.append(pltpu.roll(v, nz - 1, 0) - pltpu.roll(v, 1, 0))
            dy.append(ups[c] - downs[c])
        out[y] = tensor_norm(strain_of(dx, dy, dz))

    line = [near[0, c] * has_below for c in range(3)]
    plane(0, [velocity[c, 1] for c in range(3)], line)
    line = [near[1, c] * has_above for c in range(3)]
    plane(lp - 1, line, [velocity[c, lp - 2] for c in range(3)])

    @pl.loop(1, lp - 1)
    def _(y):
        plane(y, [velocity[c, y + 1] for c in range(3)], [velocity[c, y - 1] for c in range(3)])


def unpack_pair(held, u, slot, nz, nx):
    for c in range(3):
        turned = held[:, c, slot].reshape(nx, nx).T
        for hf in range(2):
            first = turned[2 * hf * nz : (2 * hf + 1) * nz]
            second = turned[(2 * hf + 1) * nz : (2 * hf + 2) * nz]
            u[c, hf, 2 * slot], u[c, hf, 2 * slot + 1] = swap_bit(first, second, 4)


def field_columns(u, fields, start, count, nz, nx):
    lane = lax.broadcasted_iota(jnp.int32, (nz, nx), 1)
    last, first_lane = lane % 8 == 7, lane % 8 == 0
    top, bottom = lane == nx - 1, lane == 0

    @pl.loop(0, count, unroll=2)
    def _(i):
        x = start + i
        here, dx, dy, dz = [], [], [], []
        for c in range(3):
            v = [u[c, hf, x] for hf in range(2)]
            here.append(v)
            dx.append([u[c, hf, x + 1] - u[c, hf, x - 1] for hf in range(2)])
            dz.append([pltpu.roll(v[hf], nz - 1, 0) - pltpu.roll(v[hf], 1, 0) for hf in range(2)])
            ahead = [pltpu.roll(v[hf], nx - 1, 1) for hf in range(2)]
            behind = [pltpu.roll(v[hf], 1, 1) for hf in range(2)]
            up = [
                jnp.where(last, pltpu.roll(v[1], 7, 1), ahead[0]),
                jnp.where(last, jnp.where(top, 0.0, ahead[0]), ahead[1]),
            ]
            down = [
                jnp.where(first_lane, jnp.where(bottom, 0.0, behind[1]), behind[0]),
                jnp.where(first_lane, pltpu.roll(v[0], nx - 7, 1), behind[1]),
            ]
            dy.append([up[hf] - down[hf] for hf in range(2)])
        for hf in range(2):
            gx, gy, gz = [d[hf] for d in dx], [d[hf] for d in dy], [d[hf] for d in dz]
            s = [gx[0] + gx[0], gy[1] + gy[1], gz[2] + gz[2], gy[0] + gx[1], gz[0] + gx[2], gz[1] + gy[2]]
            mag = tensor_norm(s)
            for c in range(3):
                fields[c, x, hf] = here[c][hf]
            for q, (i, j) in enumerate(PAIRS):
                fields[3 + q, x, hf] = s[q]
                fields[9 + q, x, hf] = here[i][hf] * here[j][hf]
                fields[15 + q, x, hf] = mag * s[q]


def filter_pair(fields, start, high, low, filt, wide, heavy, nz):
    cells = 2 * nz

    rows = wide.shape[1] // 2

    def box(k):
        columns = []
        for hf in range(2):
            f = [fields[k, start + i, hf] for i in range(4)]
            pair = [f[i] + f[i + 1] for i in range(3)]
            parts = []
            for i in range(2):
                along = pair[i] + pair[i + 1]
                parts.append(pltpu.roll(along, 1, 0) + pltpu.roll(along, nz - 1, 0) + (along + along))
            columns.append(jnp.concatenate(parts, axis=0))
        whole = jnp.concatenate(columns, axis=1)
        head = whole.astype(jnp.bfloat16)
        high[k * cells : (k + 1) * cells, :] = head
        low[k * cells : (k + 1) * cells, :] = (whole - head.astype(jnp.float32)).astype(jnp.bfloat16)

    dot = functools.partial(jnp.dot, preferred_element_type=jnp.float32)
    for b in range(4):
        if b < 3:
            for k in range(7 * b, 7 * b + 7):
                box(k)
        if b:
            at = slice((b - 1) * 7 * cells, b * 7 * cells)
            both = dot(high[at, :], wide[...])
            filt[at, :] = both[:, :rows] + (dot(low[at, :], heavy[...]) + both[:, rows:])


def stress_pair(filt, stress, sums, place, nz):
    cells = 2 * nz

    @pl.loop(0, cells // 8)
    def _(r):
        base = pl.multiple_of(8 * r, 8)
        g = [filt[pl.ds(base + k * cells, 8), :] for k in range(21)]
        fmag = 4.0 * tensor_norm(g[3:9])
        lm_total, mm_total = None, None
        at = pl.ds(pl.multiple_of(place * cells + base, 8), 8)
        for q, (i, j) in enumerate(PAIRS):
            leonard = g[9 + q] - g[i] * g[j]
            model = g[15 + q] - fmag * g[3 + q]
            weighted = model if q < 3 else 2.0 * model
            lm_total = leonard * weighted if q == 0 else lm_total + leonard * weighted
            mm_total = model * weighted if q == 0 else mm_total + model * weighted
            stress[q, at, :] = leonard
        sums[0] += lm_total
        sums[1] += mm_total


def flow_kernel(
    dims, velocity, inverse, block, bins, home, totals, magnitude,
    packed, held, u, fields, high, low, filt, stress, back, wide, heavy, onehot, sums, tile, beside, near,
    main_out, edge_out, pass_out, back_out, sum_out, halo_out,
    main_in, edge_in, pass_in, back_in, sum_in, halo_in,
):
    n, pairs, lp, nz, nx = dims
    ny, h = n * lp, n // 2
    strips = h // 2
    whole = 2 * pairs
    a, s = lax.axis_index("px"), lax.axis_index("pz")
    half, spot = s // h, lax.rem(s, h)
    remote = functools.partial(pltpu.make_async_remote_copy, device_id_type=MESH)
    barrier = pltpu.get_barrier_semaphore()
    me = a * n + s

    @pl.loop(1, 2 * n)
    def _(step):
        peer = lax.rem(me + step, 2 * n)
        pl.semaphore_signal(barrier, inc=1, device_id=(peer // n, lax.rem(peer, n)), device_id_type=MESH)

    pack_planes(velocity, packed)
    pl.semaphore_wait(barrier, 2 * n - 1)

    def send(source, dst, core, chip, out_sem, in_sem):
        itself = (core == a) & (chip == s)
        copy = remote(source, dst, out_sem, in_sem, device_id=(core, chip))
        return itself, copy, pltpu.make_async_copy(source, dst, in_sem)

    def start(moves):
        for itself, copy, here in moves:
            pl.when(itself)(here.start)
            pl.when(jnp.logical_not(itself))(copy.start)

    def drain(moves):
        for itself, copy, here in moves:
            pl.when(jnp.logical_not(itself))(copy.wait_send)

    def piece(pair):
        return packed.at[:, pl.ds(pl.multiple_of(8 * pair, 8), 8)]

    def edges(r):
        t, i = r // strips, lax.rem(r, strips)
        after = h * t + lax.rem(strips * a + i + 1, h)
        before = h * t + lax.rem(strips * a + i + h - 1, h)
        yield send(piece(whole * i + whole - 1), held.at[s, :, 0], 0, after, edge_out.at[0, r], edge_in.at[s])
        yield send(piece(whole * i), held.at[s, :, pairs + 1], 1, before, edge_out.at[1, r], edge_in.at[s])

    def mains(r, m):
        t, i = r // strips, lax.rem(r, strips)
        for core in range(2):
            own = m if core else pairs - 1 - m
            dst = held.at[s, :, own + 1]
            yield send(piece(whole * i + pairs * core + own), dst, core, h * t + strips * a + i, main_out.at[m, core, r], main_in.at[m, s])

    def ordered(r):
        return lax.rem(half + 1 + r // strips, 2) * strips + lax.rem(s + r, strips)

    halos = [
        remote(velocity, beside, halo_out.at[0], halo_in.at[0], device_id=(1 - a, s)),
        remote(velocity.at[:, lp - 1], near.at[0], halo_out.at[1], halo_in.at[1], device_id=(a, lax.rem(s + 1, n))),
        remote(velocity.at[:, 0], near.at[1], halo_out.at[2], halo_in.at[2], device_id=(a, lax.rem(s + n - 1, n))),
    ]
    for copy in halos:
        copy.start()

    @pl.loop(0, pairs)
    def _(m):
        @pl.loop(0, h)
        def _(r):
            start(mains(ordered(r), m))

    @pl.loop(0, h)
    def _(r):
        start(edges(ordered(r)))

    column_weights((ny, lp, nx), half == 1, inverse, block, bins, wide, heavy, onehot)
    sums[...] = jnp.zeros(sums.shape, jnp.float32)

    def slot_of(m):
        return pairs - m + a * (1 + 2 * m - pairs)

    def forward(p):
        return remote(
            held.at[p, :, slot_of(0)], held.at[p, :, (pairs + 1) * a],
            pass_out.at[p], pass_in.at[p], device_id=(1 - a, s),
        )

    def await_pair(sem, p):
        pltpu.make_async_copy(packed.at[:, 0:8], held.at[p, :, 0], sem).wait()

    mine = 2 * lax.rem(spot, strips) + a

    def returns(j, d):
        place = pairs // 2 - 1 - j + a * (1 + 2 * j - pairs // 2)
        source, dst = back.at[j, d], home.at[mine, :, place]
        return [send(source, dst, spot // strips, h * half + d, back_out.at[j, d], back_in.at[j, mine])]

    def column(m, count):
        q = slot_of(m)
        field_columns(u, fields, 2 * q - 1 if count == 4 else 2 * q - 1 + 2 * a, count, nz, nx)
        filter_pair(fields, 2 * q - 1, high, low, filt, wide, heavy, nz)
        stress_pair(filt, stress, sums, lax.rem(q - 1, 2), nz)

    def give_back(j):
        @pl.loop(0, 6)
        def _(f):
            rows = [stress[f, x * nz : (x + 1) * nz, :] for x in range(4)]
            rows[0], rows[1] = swap_bit(rows[0], rows[1], 4)
            rows[2], rows[3] = swap_bit(rows[2], rows[3], 4)
            rows[0], rows[2] = swap_bit(rows[0], rows[2], 8)
            rows[1], rows[3] = swap_bit(rows[1], rows[3], 8)
            back[j, :, f] = jnp.concatenate(rows, axis=0).T.reshape(h, lp, nx)

        for r in range(h):
            start(returns(j, flip_bits(spot, h - 1 - r, h.bit_length() - 1)))

    for copy in halos:
        copy.wait()
    plane_magnitudes(velocity, beside, near, magnitude, (s > 0).astype(jnp.float32), (s < n - 1).astype(jnp.float32))

    @pl.loop(0, n)
    def _(p):
        await_pair(main_in.at[0, p], p)
        forward(p).start()

    unpack_pair(held, u, slot_of(0), nz, nx)

    @pl.loop(0, n)
    def _(p):
        forward(p).wait()
        await_pair(main_in.at[1, p], p)

    unpack_pair(held, u, slot_of(-1), nz, nx)
    unpack_pair(held, u, slot_of(1), nz, nx)
    column(0, 4)

    @pl.loop(1, pairs)
    def _(m):
        @pl.when(m < pairs - 1)
        def _():
            @pl.loop(0, n)
            def _(p):
                await_pair(main_in.at[m + 1, p], p)

        @pl.when(m == pairs - 1)
        def _():
            @pl.loop(0, n)
            def _(p):
                await_pair(edge_in.at[p], p)

        unpack_pair(held, u, slot_of(m + 1), nz, nx)
        column(m, 2)

        @pl.when((lax.rem(m, 2) == 1) & (m < pairs - 1))
        def _():
            give_back(m // 2)

    exact = functools.partial(
        lax.dot_general, dimension_numbers=(((1,), (1,)), ((), ())),
        preferred_element_type=jnp.float32, precision=lax.Precision.HIGHEST,
    )
    spread = exact(sums[...].reshape(16, nx), onehot[...])
    tile[0:1, :] = jnp.sum(spread[0:8], axis=0, keepdims=True) * (1.0 / 16.0)
    tile[1:2, :] = jnp.sum(spread[8:16], axis=0, keepdims=True) * (1.0 / 256.0)

    def share(t):
        return [send(tile, totals.at[me], t // n, lax.rem(t, n), sum_out.at[t], sum_in.at[me])]

    @pl.loop(0, 2 * n)
    def _(r):
        start(share(lax.rem(me + r, 2 * n)))

    give_back(pairs // 2 - 1)

    @pl.loop(0, h)
    def _(r):
        drain(edges(r))

        @pl.loop(0, pairs)
        def _(m):
            drain(mains(r, m))

    @pl.loop(0, h)
    def _(p):
        for j in range(pairs // 2):
            pltpu.make_async_copy(back.at[0, 0], home.at[p, :, 0], back_in.at[j, p]).wait()
            drain(returns(j, p))

    @pl.loop(0, 2 * n)
    def _(t):
        pltpu.make_async_copy(tile, totals.at[t], sum_in.at[t]).wait()
        drain(share(t))


def finish_kernel(dims, cells, chip, home, sums, magnitude, bins, leonard, viscosity, coefficient):
    n, pairs, lp, nz, nx = dims
    ny, groups = n * lp, nx // nz
    steps = lp // groups
    total = sums[0]
    for p in range(1, 2 * n):
        total = total + sums[p]
    numer, denom = total[0:1, :], total[1:2, :]
    per_bin = numer / jnp.maximum(denom, jnp.float32(cells))
    exact = functools.partial(
        lax.dot_general, preferred_element_type=jnp.float32, precision=lax.Precision.HIGHEST
    )
    label = jnp.broadcast_to(bins[...].astype(jnp.float32), (nx, ny))
    kind = lax.broadcasted_iota(jnp.int32, (nx, ny), 0).astype(jnp.float32)
    onehot = (label == kind).astype(jnp.float32)
    table = jnp.broadcast_to(per_bin, (nx, nx))
    coefficient[...] = exact(table[0:8], onehot, (((1,), (0,)), ((), ())))[0:1, :]
    mine = jnp.zeros((nx, lp), jnp.float32)
    for s in range(n):
        mine = jnp.where(chip[0] == s, onehot[:, s * lp : (s + 1) * lp], mine)
    spread = exact(mine, table, (((0,), (1,)), ((), ())))
    for y in range(lp):
        viscosity[y] = spread[y : y + 1, :] * magnitude[y]

    for f in range(6):
        for q in range(steps):
            at = pl.ds(f * pairs * 8 + q, 2 * pairs, stride=steps)
            turned = jnp.concatenate([home[p, at, :] for p in range(nx // (2 * pairs))], axis=0).T
            for g in range(groups):
                leonard[f, g * steps + q] = turned[g * nz : (g + 1) * nz]


def by_strips(velocity, filter_inverse, filter_block, plane_bin, n):
    _, lp, nz, nx = velocity.shape
    ny, h = n * lp, n // 2
    pairs = nx // h // 2
    dims = (n, pairs, lp, nz, nx)
    steps = lp // (nx // nz)
    chip = lax.axis_index("pz").astype(jnp.int32).reshape(1)
    block = filter_block.reshape(1, ny)
    bins = plane_bin.reshape(1, ny)
    vmem = pl.BlockSpec(memory_space=pltpu.VMEM)
    smem = pl.BlockSpec(memory_space=pltpu.SMEM)
    f32 = functools.partial(jax.ShapeDtypeStruct, dtype=jnp.float32)
    dma = pltpu.SemaphoreType.DMA

    room = functools.partial(pltpu.VMEM, dtype=jnp.float32)
    home, sums, magnitude = pl.pallas_call(
        functools.partial(flow_kernel, dims),
        out_shape=(f32((h, 6, pairs // 2, lp, nx)), f32((2 * n, 2, nx)), f32((lp, nz, nx))),
        in_specs=[vmem] * 4,
        out_specs=(vmem,) * 3,
        scratch_shapes=[
            room((3, nx * steps, nx)),
            room((n, 3, pairs + 2, 8, nx)),
            room((3, 2, 2 * pairs + 4, nz, nx)),
            room((21, 2 * pairs + 4, 2, nz, nx)),
            pltpu.VMEM((21 * 2 * nz, ny), jnp.bfloat16),
            pltpu.VMEM((21 * 2 * nz, ny), jnp.bfloat16),
            room((21 * 2 * nz, ny // 2)),
            room((6, 4 * nz, nx)),
            room((pairs // 2, h, 6, lp, nx)),
            pltpu.VMEM((ny, ny), jnp.bfloat16),
            pltpu.VMEM((ny, ny // 2), jnp.bfloat16),
            room((nx, ny // 2)),
            room((2, 8, ny // 2)),
            room((2, nx)),
            room((3, lp, nz, nx)),
            room((2, 3, nz, nx)),
            dma((pairs, 2, h)),
            dma((2, h)),
            dma((n,)),
            dma((pairs // 2, h)),
            dma((2 * n,)),
            dma((3,)),
            dma((pairs, n)),
            dma((n,)),
            dma((n,)),
            dma((pairs // 2, h)),
            dma((2 * n,)),
            dma((3,)),
        ],
        compiler_params=pltpu.CompilerParams(
            collective_id=0, has_side_effects=True, vmem_limit_bytes=60 * 1024 * 1024
        ),
    )(velocity, filter_inverse, block, bins)
    home = home.reshape(h, 6 * pairs // 2 * lp, nx)
    leonard, viscosity, coefficient = pl.pallas_call(
        functools.partial(finish_kernel, dims, 2 * nx * nz),
        out_shape=(f32((6, lp, nz, nx)), f32((lp, nz, nx)), f32((1, ny))),
        in_specs=[smem] + [vmem] * 4,
        out_specs=(vmem,) * 3,
    )(chip, home, sums, magnitude, bins)
    return (leonard, viscosity, coefficient.reshape(ny))


def by_blocks(velocity, filter_inverse, filter_block, plane_bin):
    _, lp, nz, nx = velocity.shape
    n = lax.axis_size("pz")
    m = lax.axis_size("px")
    ny, zs = n * lp, nz // n
    win = zs + 4

    same = (filter_block[:, None] == filter_block[None, :]).astype(jnp.float32)
    masked = filter_inverse * same
    weights = masked / jnp.sum(masked, axis=1, keepdims=True)
    onehot = (plane_bin[:, None] == jnp.arange(nx, dtype=jnp.int32)[None, :]).astype(jnp.float32)

    right = lax.ppermute(velocity, "px", [((i + 1) % m, i) for i in range(m)])
    left = right if m == 2 else lax.ppermute(velocity, "px", [(i, (i + 1) % m) for i in range(m)])
    below = lax.ppermute(velocity[:, -1:], "pz", [(i, i + 1) for i in range(n - 1)])
    above = lax.ppermute(velocity[:, :1], "pz", [(i + 1, i) for i in range(n - 1)])
    magnitude = pl.pallas_call(
        magnitude_kernel,
        out_shape=jax.ShapeDtypeStruct((lp, nz, nx), jnp.float32),
        cost_estimate=pl.CostEstimate(flops=60 * lp * nz * nx, bytes_accessed=40 * lp * nz * nx, transcendentals=0),
    )(velocity, right, left, below, above)
    turned = jnp.transpose(velocity, (0, 2, 1, 3))
    turned = jnp.concatenate([turned[:, -2:], turned, turned[:, :2]], axis=1)
    sent = jnp.stack([turned[:, t * zs : t * zs + win] for t in range(n)])
    own = lax.all_to_all(sent, "pz", split_axis=0, concat_axis=0, tiled=True)
    ahead = lax.ppermute(own, "px", [((i + 1) % m, i) for i in range(m)])
    behind = lax.ppermute(own, "px", [(i, (i + 1) % m) for i in range(m)])
    blocks = (own, ahead, behind)

    rows = 6 * zs * lp
    back = pl.pallas_call(
        functools.partial(column_kernel, (n, win, lp, nx), fill_from_blocks, len(blocks)),
        out_shape=jax.ShapeDtypeStruct((n, rows + 8, nx), jnp.float32),
        in_specs=[pl.BlockSpec(memory_space=pltpu.VMEM)] * 5,
        out_specs=pl.BlockSpec(memory_space=pltpu.VMEM),
        scratch_shapes=[
            pltpu.VMEM((3, win, ny + 16, 2 * nx), jnp.float32),
            pltpu.VMEM((21, ny, zs * nx), jnp.bfloat16),
            pltpu.VMEM((21, ny, zs * nx), jnp.bfloat16),
            pltpu.VMEM((21, ny, zs * nx), jnp.float32),
            pltpu.VMEM((ny, nx), jnp.float32),
            pltpu.VMEM((ny, nx), jnp.float32),
            pltpu.VMEM((ny, ny), jnp.bfloat16),
            pltpu.VMEM((ny, ny), jnp.bfloat16),
        ],
        compiler_params=pltpu.CompilerParams(vmem_limit_bytes=60 * 1024 * 1024),
    )(*blocks, weights, onehot)

    home = lax.all_to_all(back, "pz", split_axis=0, concat_axis=0, tiled=True)
    totals = lax.psum(jnp.sum(home[:, rows:], axis=0), "px")
    stress = home[:, :rows].reshape(n, 6, zs, lp, nx)
    leonard = jnp.transpose(stress, (1, 3, 0, 2, 4)).reshape(6, lp, nz, nx)
    numer, denom = totals[0, :NBIN], totals[4, :NBIN]
    cells = nx * m * nz
    per_bin = numer / jnp.maximum(denom, jnp.float32(cells))
    coefficient = jnp.dot(onehot[:, :NBIN], per_bin, precision=lax.Precision.HIGHEST)
    local_coef = lax.dynamic_slice_in_dim(coefficient, lax.axis_index("pz") * lp, lp, 0)
    viscosity = local_coef[:, None, None] * magnitude
    return (leonard, viscosity, coefficient)


def local(*arrays):
    _, lp, nz, nx = arrays[0].shape
    n, m = lax.axis_size("pz"), lax.axis_size("px")
    groups = nx // nz
    fits = m == 2 and n % 4 == 0 and 8 * n == nx and groups * nz == nx and lp == 16 and groups == 4
    if fits:
        return by_strips(*arrays, n)
    return by_blocks(*arrays)


def solution(mesh):
    return jax.shard_map(
        local,
        mesh=mesh,
        in_specs=(P(None, "pz", None, "px"), P(), P(), P()),
        out_specs=(P(None, "pz", None, "px"), P("pz", None, "px"), P()),
        check_vma=False,
    )
```

```python
import functools

import jax
import jax.numpy as jnp
from jax import lax
from jax.experimental import pallas as pl
from jax.experimental.pallas import tpu as pltpu
from jax.sharding import PartitionSpec as P

NBIN = 64
MESH = pl.DeviceIdType.MESH
PAIRS = ((0, 0), (1, 1), (2, 2), (0, 1), (0, 2), (1, 2))


def tensor_norm(s):
    diag = s[0] * s[0] + s[1] * s[1] + s[2] * s[2]
    off = s[3] * s[3] + s[4] * s[4] + s[5] * s[5]
    return jnp.sqrt(2.0 * diag + 4.0 * off)


def strain_of(dx, dy, dz):
    return [
        dx[0] * 0.5,
        dy[1] * 0.5,
        dz[2] * 0.5,
        0.25 * (dy[0] + dx[1]),
        0.25 * (dz[0] + dx[2]),
        0.25 * (dz[1] + dy[2]),
    ]


def fill_from_blocks(dims, ext, own, right, left):
    n, win, lp, nx = dims
    lane = lax.broadcasted_iota(jnp.int32, (lp, nx), 1)
    from_right = lane < nx // 2

    @pl.loop(0, n)
    def _(p):
        rows = pl.ds(pl.multiple_of(8 + p * lp, 8), lp)
        for c in range(3):
            for z in range(win):
                ext[c, z, rows, 0:nx] = own[p, c, z]
                ext[c, z, rows, nx : 2 * nx] = jnp.where(from_right, right[p, c, z], left[p, c, z])


def column_kernel(dims, fill, sources, *refs):
    n, win, lp, nx = dims
    blocks, refs = refs[:sources], refs[sources:]
    weights, onehot, back, ext, bhi, blo, filt, lms, mms, whi, wlo = refs
    zs = win - 4
    ny = n * lp
    lanes = 2 * nx
    heavy = weights[...].astype(jnp.bfloat16)
    whi[...] = heavy
    wlo[...] = (weights[...] - heavy.astype(jnp.float32)).astype(jnp.bfloat16)

    zero = jnp.zeros((8, lanes), jnp.float32)
    for c in range(3):
        for z in range(win):
            ext[c, z, 0:8, :] = zero
            ext[c, z, ny + 8 : ny + 16, :] = zero
    fill(dims, ext, *blocks)

    @pl.loop(0, n)
    def _(p):
        base = pl.multiple_of(p * lp, 8)
        u = [[ext[c, z, pl.ds(base + 8, lp), :] for z in range(win)] for c in range(3)]
        boxes = [[None] * 21 for _ in range(zs)]
        for z in range(1, win - 1):
            v = [u[c][z] for c in range(3)]
            dx, dy, dz = [], [], []
            for c in range(3):
                dx.append(pltpu.roll(v[c], lanes - 1, 1) - pltpu.roll(v[c], 1, 1))
                tall = ext[c, z, pl.ds(base, lp + 16), :]
                dy.append(tall[9 : 9 + lp] - tall[7 : 7 + lp])
                dz.append(u[c][z + 1] - u[c][z - 1])
            s = strain_of(dx, dy, dz)
            mag = tensor_norm(s)
            fields = v + s + [v[i] * v[j] for i, j in PAIRS] + [mag * t for t in s]
            for o in range(zs):
                step = z - (o + 2)
                if -1 <= step <= 1:
                    for k in range(21):
                        term = fields[k] if step else 2.0 * fields[k]
                        boxes[o][k] = term if boxes[o][k] is None else boxes[o][k] + term
        for o in range(zs):
            for k in range(21):
                f = boxes[o][k]
                box = (pltpu.roll(f, 1, 1) + pltpu.roll(f, lanes - 1, 1) + 2.0 * f)[:, :nx] * 0.0625
                high = box.astype(jnp.bfloat16)
                cols = slice(o * nx, (o + 1) * nx)
                bhi[k, pl.ds(base, lp), cols] = high
                blo[k, pl.ds(base, lp), cols] = (box - high.astype(jnp.float32)).astype(jnp.bfloat16)

    @pl.loop(0, 21)
    def _(k):
        dot = functools.partial(jnp.dot, preferred_element_type=jnp.float32)
        filt[k] = dot(whi[...], bhi[k]) + (dot(whi[...], blo[k]) + dot(wlo[...], bhi[k]))

    @pl.loop(0, n)
    def _(p):
        base = pl.multiple_of(p * lp, 8)
        lm_total = jnp.zeros((lp, nx), jnp.float32)
        mm_total = jnp.zeros((lp, nx), jnp.float32)
        for o in range(zs):
            g = [filt[k, pl.ds(base, lp), o * nx : (o + 1) * nx] for k in range(21)]
            fmag = 4.0 * tensor_norm(g[3:9])
            for q, (i, j) in enumerate(PAIRS):
                leonard = g[9 + q] - g[i] * g[j]
                model = g[15 + q] - fmag * g[3 + q]
                weighted = model if q < 3 else 2.0 * model
                lm_total += leonard * weighted
                mm_total += model * weighted
                back[p, (q * zs + o) * lp : (q * zs + o + 1) * lp, :] = leonard
        lms[pl.ds(base, lp), :] = lm_total
        mms[pl.ds(base, lp), :] = mm_total

    ones = jnp.ones((8, nx), jnp.float32)
    exact = functools.partial(
        lax.dot_general, preferred_element_type=jnp.float32, precision=lax.Precision.HIGHEST
    )
    totals = []
    for part in (lms, mms):
        planes = exact(ones, part[...], (((1,), (1,)), ((), ())))
        totals.append(exact(planes, onehot[...], (((1,), (0,)), ((), ()))))
    row = lax.broadcasted_iota(jnp.int32, (8, onehot.shape[1]), 0)
    tile = jnp.where(row < 4, totals[0], totals[1])
    for p in range(n):
        back[p, 6 * zs * lp :, :] = tile


def greet_all(m, n):
    me = lax.axis_index("px") * n + lax.axis_index("pz")
    barrier = pltpu.get_barrier_semaphore()

    @pl.loop(1, m * n)
    def _(step):
        peer = lax.rem(me + step, m * n)
        pl.semaphore_signal(barrier, inc=1, device_id=(peer // n, lax.rem(peer, n)), device_id_type=MESH)

    pl.semaphore_wait(barrier, m * n - 1)


def magnitude_kernel(centre, right, left, below, above, out):
    _, lp, nz, nx = centre.shape
    lane = lax.broadcasted_iota(jnp.int32, (nz, nx), 1)
    for y in range(lp):
        v = [centre[c, y] for c in range(3)]
        dx, dy, dz = [], [], []
        for c in range(3):
            ahead = jnp.where(lane == nx - 1, pltpu.roll(right[c, y], nx - 1, 1), pltpu.roll(v[c], nx - 1, 1))
            behind = jnp.where(lane == 0, pltpu.roll(left[c, y], 1, 1), pltpu.roll(v[c], 1, 1))
            dx.append(ahead - behind)
            dz.append(pltpu.roll(v[c], nz - 1, 0) - pltpu.roll(v[c], 1, 0))
            up = centre[c, y + 1] if y + 1 < lp else above[c, 0]
            down = centre[c, y - 1] if y else below[c, 0]
            dy.append(up - down)
        out[y] = tensor_norm(strain_of(dx, dy, dz))


def swap_bit(first, second, bit):
    nx = first.shape[-1]
    low = (lax.broadcasted_iota(jnp.int32, first.shape, 1) & bit) == 0
    return (
        jnp.where(low, first, pltpu.roll(second, bit, 1)),
        jnp.where(low, pltpu.roll(first, nx - bit, 1), second),
    )


def pack_planes(velocity, packed):
    _, lp, nz, nx = velocity.shape
    groups = nx // nz
    steps = lp // groups
    for c in range(3):
        for q in range(steps):
            rows = jnp.concatenate([velocity[c, g * steps + q] for g in range(groups)], axis=0)
            packed[c, pl.ds(q, nx, stride=steps), :] = rows.T


def plane_order(shape, lp, nx, dim):
    at = lax.broadcasted_iota(jnp.int32, shape, dim)
    return (at % nx) // 8 * lp + at // nx * 8 + at % 8


def column_weights(dims, upper, inverse, block, bins, wide, heavy, onehot):
    ny, lp, nx = dims
    rows = ny // 2
    label = jnp.broadcast_to(block[...].astype(jnp.float32), (ny, ny))
    turned = label.T
    mine = jnp.where(upper, turned[rows:], turned[:rows])
    masked = jnp.where(label[:rows] == mine, jnp.where(upper, inverse[rows:, :], inverse[:rows, :]), 0.0)
    weights = masked / jnp.sum(masked, axis=1, keepdims=True) * 0.0625
    order = plane_order((ny, ny), lp, nx, 0) == lax.broadcasted_iota(jnp.int32, (ny, ny), 1)
    order = order.astype(jnp.float32).astype(jnp.bfloat16)

    def placed(part):
        dims = (((1,), (1,)), ((), ()))
        return lax.dot_general(order, part, dims, preferred_element_type=jnp.float32).astype(jnp.bfloat16)

    head = weights.astype(jnp.bfloat16)
    rest = (weights - head.astype(jnp.float32)).astype(jnp.bfloat16)
    heavy[...] = placed(head)
    wide[:, :rows] = heavy[...]
    wide[:, rows:] = placed(rest)
    label = jnp.where(upper, bins[:, rows:], bins[:, :rows])
    kind = lax.broadcasted_iota(jnp.int32, (nx, rows), 0)
    onehot[...] = (jnp.broadcast_to(label, (nx, rows)) == kind).astype(jnp.float32)


def flip_bits(value, mask, count):
    out = 0
    for bit in range(count):
        digit = lax.rem(value // (1 << bit), 2)
        out = out + (1 << bit) * ((1 - digit) if mask >> bit & 1 else digit)
    return out


def plane_magnitudes(velocity, beside, near, out, has_below, has_above):
    _, lp, nz, nx = velocity.shape
    lane = lax.broadcasted_iota(jnp.int32, (nz, nx), 1)

    def plane(y, ups, downs):
        dx, dy, dz = [], [], []
        for c in range(3):
            v, side = velocity[c, y], beside[c, y]
            ahead = jnp.where(lane == nx - 1, pltpu.roll(side, nx - 1, 1), pltpu.roll(v, nx - 1, 1))
            behind = jnp.where(lane == 0, pltpu.roll(side, 1, 1), pltpu.roll(v, 1, 1))
            dx.append(ahead - behind)
            dz.append(pltpu.roll(v, nz - 1, 0) - pltpu.roll(v, 1, 0))
            dy.append(ups[c] - downs[c])
        out[y] = tensor_norm(strain_of(dx, dy, dz))

    line = [near[0, c] * has_below for c in range(3)]
    plane(0, [velocity[c, 1] for c in range(3)], line)
    line = [near[1, c] * has_above for c in range(3)]
    plane(lp - 1, line, [velocity[c, lp - 2] for c in range(3)])

    @pl.loop(1, lp - 1)
    def _(y):
        plane(y, [velocity[c, y + 1] for c in range(3)], [velocity[c, y - 1] for c in range(3)])


def unpack_pair(held, u, slot, nz, nx):
    for c in range(3):
        turned = held[:, c, slot].reshape(nx, nx).T
        for hf in range(2):
            first = turned[2 * hf * nz : (2 * hf + 1) * nz]
            second = turned[(2 * hf + 1) * nz : (2 * hf + 2) * nz]
            u[c, hf, 2 * slot], u[c, hf, 2 * slot + 1] = swap_bit(first, second, 4)


def field_columns(u, fields, start, count, nz, nx):
    lane = lax.broadcasted_iota(jnp.int32, (nz, nx), 1)
    last, first_lane = lane % 8 == 7, lane % 8 == 0
    top, bottom = lane == nx - 1, lane == 0

    @pl.loop(0, count, unroll=2)
    def _(i):
        x = start + i
        here, dx, dy, dz = [], [], [], []
        for c in range(3):
            v = [u[c, hf, x] for hf in range(2)]
            here.append(v)
            dx.append([u[c, hf, x + 1] - u[c, hf, x - 1] for hf in range(2)])
            dz.append([pltpu.roll(v[hf], nz - 1, 0) - pltpu.roll(v[hf], 1, 0) for hf in range(2)])
            ahead = [pltpu.roll(v[hf], nx - 1, 1) for hf in range(2)]
            behind = [pltpu.roll(v[hf], 1, 1) for hf in range(2)]
            up = [
                jnp.where(last, pltpu.roll(v[1], 7, 1), ahead[0]),
                jnp.where(last, jnp.where(top, 0.0, ahead[0]), ahead[1]),
            ]
            down = [
                jnp.where(first_lane, jnp.where(bottom, 0.0, behind[1]), behind[0]),
                jnp.where(first_lane, pltpu.roll(v[0], nx - 7, 1), behind[1]),
            ]
            dy.append([up[hf] - down[hf] for hf in range(2)])
        for hf in range(2):
            gx, gy, gz = [d[hf] for d in dx], [d[hf] for d in dy], [d[hf] for d in dz]
            s = [gx[0] + gx[0], gy[1] + gy[1], gz[2] + gz[2], gy[0] + gx[1], gz[0] + gx[2], gz[1] + gy[2]]
            mag = tensor_norm(s)
            for c in range(3):
                fields[c, x, hf] = here[c][hf]
            for q, (i, j) in enumerate(PAIRS):
                fields[3 + q, x, hf] = s[q]
                fields[9 + q, x, hf] = here[i][hf] * here[j][hf]
                fields[15 + q, x, hf] = mag * s[q]


def filter_pair(fields, start, high, low, filt, wide, heavy, nz):
    cells = 2 * nz

    rows = wide.shape[1] // 2

    def box(k):
        columns = []
        for hf in range(2):
            f = [fields[k, start + i, hf] for i in range(4)]
            pair = [f[i] + f[i + 1] for i in range(3)]
            parts = []
            for i in range(2):
                along = pair[i] + pair[i + 1]
                parts.append(pltpu.roll(along, 1, 0) + pltpu.roll(along, nz - 1, 0) + (along + along))
            columns.append(jnp.concatenate(parts, axis=0))
        whole = jnp.concatenate(columns, axis=1)
        head = whole.astype(jnp.bfloat16)
        high[k * cells : (k + 1) * cells, :] = head
        low[k * cells : (k + 1) * cells, :] = (whole - head.astype(jnp.float32)).astype(jnp.bfloat16)

    dot = functools.partial(jnp.dot, preferred_element_type=jnp.float32)
    for b in range(4):
        if b < 3:
            for k in range(7 * b, 7 * b + 7):
                box(k)
        if b:
            at = slice((b - 1) * 7 * cells, b * 7 * cells)
            both = dot(high[at, :], wide[...])
            filt[at, :] = both[:, :rows] + (dot(low[at, :], heavy[...]) + both[:, rows:])


def stress_pair(filt, stress, sums, place, nz):
    cells = 2 * nz

    @pl.loop(0, cells // 8)
    def _(r):
        base = pl.multiple_of(8 * r, 8)
        g = [filt[pl.ds(base + k * cells, 8), :] for k in range(21)]
        fmag = 4.0 * tensor_norm(g[3:9])
        lm_total, mm_total = None, None
        at = pl.ds(pl.multiple_of(place * cells + base, 8), 8)
        for q, (i, j) in enumerate(PAIRS):
            leonard = g[9 + q] - g[i] * g[j]
            model = g[15 + q] - fmag * g[3 + q]
            weighted = model if q < 3 else 2.0 * model
            lm_total = leonard * weighted if q == 0 else lm_total + leonard * weighted
            mm_total = model * weighted if q == 0 else mm_total + model * weighted
            stress[q, at, :] = leonard
        sums[0] += lm_total
        sums[1] += mm_total


def flow_kernel(
    dims, velocity, inverse, block, bins, home, totals, magnitude,
    packed, held, u, fields, high, low, filt, stress, back, wide, heavy, onehot, sums, tile, beside, near,
    main_out, edge_out, pass_out, back_out, sum_out, halo_out,
    main_in, edge_in, pass_in, back_in, sum_in, halo_in,
):
    n, pairs, lp, nz, nx = dims
    ny, h = n * lp, n // 2
    strips = h // 2
    whole = 2 * pairs
    a, s = lax.axis_index("px"), lax.axis_index("pz")
    half, spot = s // h, lax.rem(s, h)
    remote = functools.partial(pltpu.make_async_remote_copy, device_id_type=MESH)
    barrier = pltpu.get_barrier_semaphore()
    me = a * n + s

    @pl.loop(1, 2 * n)
    def _(step):
        peer = lax.rem(me + step, 2 * n)
        pl.semaphore_signal(barrier, inc=1, device_id=(peer // n, lax.rem(peer, n)), device_id_type=MESH)

    pack_planes(velocity, packed)
    pl.semaphore_wait(barrier, 2 * n - 1)

    def send(source, dst, core, chip, out_sem, in_sem):
        itself = (core == a) & (chip == s)
        copy = remote(source, dst, out_sem, in_sem, device_id=(core, chip))
        return itself, copy, pltpu.make_async_copy(source, dst, in_sem)

    def start(moves):
        for itself, copy, here in moves:
            pl.when(itself)(here.start)
            pl.when(jnp.logical_not(itself))(copy.start)

    def drain(moves):
        for itself, copy, here in moves:
            pl.when(jnp.logical_not(itself))(copy.wait_send)

    def piece(pair):
        return packed.at[:, pl.ds(pl.multiple_of(8 * pair, 8), 8)]

    def edges(r):
        t, i = r // strips, lax.rem(r, strips)
        after = h * t + lax.rem(strips * a + i + 1, h)
        before = h * t + lax.rem(strips * a + i + h - 1, h)
        yield send(piece(whole * i + whole - 1), held.at[s, :, 0], 0, after, edge_out.at[0, r], edge_in.at[s])
        yield send(piece(whole * i), held.at[s, :, pairs + 1], 1, before, edge_out.at[1, r], edge_in.at[s])

    def mains(r, m):
        t, i = r // strips, lax.rem(r, strips)
        for core in range(2):
            own = m if core else pairs - 1 - m
            dst = held.at[s, :, own + 1]
            yield send(piece(whole * i + pairs * core + own), dst, core, h * t + strips * a + i, main_out.at[m, core, r], main_in.at[m, s])

    def ordered(r):
        return lax.rem(half + 1 + r // strips, 2) * strips + lax.rem(s + r, strips)

    halos = [
        remote(velocity, beside, halo_out.at[0], halo_in.at[0], device_id=(1 - a, s)),
        remote(velocity.at[:, lp - 1], near.at[0], halo_out.at[1], halo_in.at[1], device_id=(a, lax.rem(s + 1, n))),
        remote(velocity.at[:, 0], near.at[1], halo_out.at[2], halo_in.at[2], device_id=(a, lax.rem(s + n - 1, n))),
    ]
    for copy in halos:
        copy.start()

    @pl.loop(0, pairs)
    def _(m):
        @pl.loop(0, h)
        def _(r):
            start(mains(ordered(r), m))

    @pl.loop(0, h)
    def _(r):
        start(edges(ordered(r)))

    column_weights((ny, lp, nx), half == 1, inverse, block, bins, wide, heavy, onehot)
    sums[...] = jnp.zeros(sums.shape, jnp.float32)

    def slot_of(m):
        return pairs - m + a * (1 + 2 * m - pairs)

    def forward(p):
        return remote(
            held.at[p, :, slot_of(0)], held.at[p, :, (pairs + 1) * a],
            pass_out.at[p], pass_in.at[p], device_id=(1 - a, s),
        )

    def await_pair(sem, p):
        pltpu.make_async_copy(packed.at[:, 0:8], held.at[p, :, 0], sem).wait()

    mine = 2 * lax.rem(spot, strips) + a

    def returns(j, d):
        place = pairs // 2 - 1 - j + a * (1 + 2 * j - pairs // 2)
        source, dst = back.at[j, d], home.at[mine, :, place]
        return [send(source, dst, spot // strips, h * half + d, back_out.at[j, d], back_in.at[j, mine])]

    def column(m, count):
        q = slot_of(m)
        field_columns(u, fields, 2 * q - 1 if count == 4 else 2 * q - 1 + 2 * a, count, nz, nx)
        filter_pair(fields, 2 * q - 1, high, low, filt, wide, heavy, nz)
        stress_pair(filt, stress, sums, lax.rem(q - 1, 2), nz)

    def give_back(j):
        for f in range(6):
            rows = [stress[f, x * nz : (x + 1) * nz, :] for x in range(4)]
            rows[0], rows[1] = swap_bit(rows[0], rows[1], 4)
            rows[2], rows[3] = swap_bit(rows[2], rows[3], 4)
            rows[0], rows[2] = swap_bit(rows[0], rows[2], 8)
            rows[1], rows[3] = swap_bit(rows[1], rows[3], 8)
            back[j, :, f] = jnp.concatenate(rows, axis=0).T.reshape(h, lp, nx)

        for r in range(h):
            start(returns(j, flip_bits(spot, h - 1 - r, h.bit_length() - 1)))

    for copy in halos:
        copy.wait()
    plane_magnitudes(velocity, beside, near, magnitude, (s > 0).astype(jnp.float32), (s < n - 1).astype(jnp.float32))

    @pl.loop(0, n)
    def _(p):
        await_pair(main_in.at[0, p], p)
        forward(p).start()

    unpack_pair(held, u, slot_of(0), nz, nx)

    @pl.loop(0, n)
    def _(p):
        forward(p).wait()
        await_pair(main_in.at[1, p], p)

    unpack_pair(held, u, slot_of(-1), nz, nx)
    unpack_pair(held, u, slot_of(1), nz, nx)
    column(0, 4)

    @pl.loop(1, pairs)
    def _(m):
        @pl.when(m < pairs - 1)
        def _():
            @pl.loop(0, n)
            def _(p):
                await_pair(main_in.at[m + 1, p], p)

        @pl.when(m == pairs - 1)
        def _():
            @pl.loop(0, n)
            def _(p):
                await_pair(edge_in.at[p], p)

        unpack_pair(held, u, slot_of(m + 1), nz, nx)
        column(m, 2)

        @pl.when((lax.rem(m, 2) == 1) & (m < pairs - 1))
        def _():
            give_back(m // 2)

    exact = functools.partial(
        lax.dot_general, dimension_numbers=(((1,), (1,)), ((), ())),
        preferred_element_type=jnp.float32, precision=lax.Precision.HIGHEST,
    )
    spread = exact(sums[...].reshape(16, nx), onehot[...])
    tile[0:1, :] = jnp.sum(spread[0:8], axis=0, keepdims=True) * (1.0 / 16.0)
    tile[1:2, :] = jnp.sum(spread[8:16], axis=0, keepdims=True) * (1.0 / 256.0)

    def share(t):
        return [send(tile, totals.at[me], t // n, lax.rem(t, n), sum_out.at[t], sum_in.at[me])]

    @pl.loop(0, 2 * n)
    def _(r):
        start(share(lax.rem(me + r, 2 * n)))

    give_back(pairs // 2 - 1)

    @pl.loop(0, h)
    def _(r):
        drain(edges(r))

        @pl.loop(0, pairs)
        def _(m):
            drain(mains(r, m))

    @pl.loop(0, h)
    def _(p):
        for j in range(pairs // 2):
            pltpu.make_async_copy(back.at[0, 0], home.at[p, :, 0], back_in.at[j, p]).wait()
            drain(returns(j, p))

    @pl.loop(0, 2 * n)
    def _(t):
        pltpu.make_async_copy(tile, totals.at[t], sum_in.at[t]).wait()
        drain(share(t))


def finish_kernel(dims, cells, chip, home, sums, magnitude, bins, leonard, viscosity, coefficient):
    n, pairs, lp, nz, nx = dims
    ny, groups = n * lp, nx // nz
    steps = lp // groups
    total = sums[0]
    for p in range(1, 2 * n):
        total = total + sums[p]
    numer, denom = total[0:1, :], total[1:2, :]
    per_bin = numer / jnp.maximum(denom, jnp.float32(cells))
    exact = functools.partial(
        lax.dot_general, preferred_element_type=jnp.float32, precision=lax.Precision.HIGHEST
    )
    label = jnp.broadcast_to(bins[...].astype(jnp.float32), (nx, ny))
    kind = lax.broadcasted_iota(jnp.int32, (nx, ny), 0).astype(jnp.float32)
    onehot = (label == kind).astype(jnp.float32)
    table = jnp.broadcast_to(per_bin, (nx, nx))
    coefficient[...] = exact(table[0:8], onehot, (((1,), (0,)), ((), ())))[0:1, :]
    mine = jnp.zeros((nx, lp), jnp.float32)
    for s in range(n):
        mine = jnp.where(chip[0] == s, onehot[:, s * lp : (s + 1) * lp], mine)
    spread = exact(mine, table, (((0,), (1,)), ((), ())))
    for y in range(lp):
        viscosity[y] = spread[y : y + 1, :] * magnitude[y]

    for f in range(6):
        for q in range(steps):
            at = pl.ds(f * pairs * 8 + q, 2 * pairs, stride=steps)
            turned = jnp.concatenate([home[p, at, :] for p in range(nx // (2 * pairs))], axis=0).T
            for g in range(groups):
                leonard[f, g * steps + q] = turned[g * nz : (g + 1) * nz]


def by_strips(velocity, filter_inverse, filter_block, plane_bin, n):
    _, lp, nz, nx = velocity.shape
    ny, h = n * lp, n // 2
    pairs = nx // h // 2
    dims = (n, pairs, lp, nz, nx)
    steps = lp // (nx // nz)
    chip = lax.axis_index("pz").astype(jnp.int32).reshape(1)
    block = filter_block.reshape(1, ny)
    bins = plane_bin.reshape(1, ny)
    vmem = pl.BlockSpec(memory_space=pltpu.VMEM)
    smem = pl.BlockSpec(memory_space=pltpu.SMEM)
    f32 = functools.partial(jax.ShapeDtypeStruct, dtype=jnp.float32)
    dma = pltpu.SemaphoreType.DMA

    room = functools.partial(pltpu.VMEM, dtype=jnp.float32)
    home, sums, magnitude = pl.pallas_call(
        functools.partial(flow_kernel, dims),
        out_shape=(f32((h, 6, pairs // 2, lp, nx)), f32((2 * n, 2, nx)), f32((lp, nz, nx))),
        in_specs=[vmem] * 4,
        out_specs=(vmem,) * 3,
        scratch_shapes=[
            room((3, nx * steps, nx)),
            room((n, 3, pairs + 2, 8, nx)),
            room((3, 2, 2 * pairs + 4, nz, nx)),
            room((21, 2 * pairs + 4, 2, nz, nx)),
            pltpu.VMEM((21 * 2 * nz, ny), jnp.bfloat16),
            pltpu.VMEM((21 * 2 * nz, ny), jnp.bfloat16),
            room((21 * 2 * nz, ny // 2)),
            room((6, 4 * nz, nx)),
            room((pairs // 2, h, 6, lp, nx)),
            pltpu.VMEM((ny, ny), jnp.bfloat16),
            pltpu.VMEM((ny, ny // 2), jnp.bfloat16),
            room((nx, ny // 2)),
            room((2, 8, ny // 2)),
            room((2, nx)),
            room((3, lp, nz, nx)),
            room((2, 3, nz, nx)),
            dma((pairs, 2, h)),
            dma((2, h)),
            dma((n,)),
            dma((pairs // 2, h)),
            dma((2 * n,)),
            dma((3,)),
            dma((pairs, n)),
            dma((n,)),
            dma((n,)),
            dma((pairs // 2, h)),
            dma((2 * n,)),
            dma((3,)),
        ],
        compiler_params=pltpu.CompilerParams(
            collective_id=0, has_side_effects=True, vmem_limit_bytes=60 * 1024 * 1024
        ),
    )(velocity, filter_inverse, block, bins)
    home = home.reshape(h, 6 * pairs // 2 * lp, nx)
    leonard, viscosity, coefficient = pl.pallas_call(
        functools.partial(finish_kernel, dims, 2 * nx * nz),
        out_shape=(f32((6, lp, nz, nx)), f32((lp, nz, nx)), f32((1, ny))),
        in_specs=[smem] + [vmem] * 4,
        out_specs=(vmem,) * 3,
    )(chip, home, sums, magnitude, bins)
    return (leonard, viscosity, coefficient.reshape(ny))


def by_blocks(velocity, filter_inverse, filter_block, plane_bin):
    _, lp, nz, nx = velocity.shape
    n = lax.axis_size("pz")
    m = lax.axis_size("px")
    ny, zs = n * lp, nz // n
    win = zs + 4

    same = (filter_block[:, None] == filter_block[None, :]).astype(jnp.float32)
    masked = filter_inverse * same
    weights = masked / jnp.sum(masked, axis=1, keepdims=True)
    onehot = (plane_bin[:, None] == jnp.arange(nx, dtype=jnp.int32)[None, :]).astype(jnp.float32)

    right = lax.ppermute(velocity, "px", [((i + 1) % m, i) for i in range(m)])
    left = right if m == 2 else lax.ppermute(velocity, "px", [(i, (i + 1) % m) for i in range(m)])
    below = lax.ppermute(velocity[:, -1:], "pz", [(i, i + 1) for i in range(n - 1)])
    above = lax.ppermute(velocity[:, :1], "pz", [(i + 1, i) for i in range(n - 1)])
    magnitude = pl.pallas_call(
        magnitude_kernel,
        out_shape=jax.ShapeDtypeStruct((lp, nz, nx), jnp.float32),
        cost_estimate=pl.CostEstimate(flops=60 * lp * nz * nx, bytes_accessed=40 * lp * nz * nx, transcendentals=0),
    )(velocity, right, left, below, above)
    turned = jnp.transpose(velocity, (0, 2, 1, 3))
    turned = jnp.concatenate([turned[:, -2:], turned, turned[:, :2]], axis=1)
    sent = jnp.stack([turned[:, t * zs : t * zs + win] for t in range(n)])
    own = lax.all_to_all(sent, "pz", split_axis=0, concat_axis=0, tiled=True)
    ahead = lax.ppermute(own, "px", [((i + 1) % m, i) for i in range(m)])
    behind = lax.ppermute(own, "px", [(i, (i + 1) % m) for i in range(m)])
    blocks = (own, ahead, behind)

    rows = 6 * zs * lp
    back = pl.pallas_call(
        functools.partial(column_kernel, (n, win, lp, nx), fill_from_blocks, len(blocks)),
        out_shape=jax.ShapeDtypeStruct((n, rows + 8, nx), jnp.float32),
        in_specs=[pl.BlockSpec(memory_space=pltpu.VMEM)] * 5,
        out_specs=pl.BlockSpec(memory_space=pltpu.VMEM),
        scratch_shapes=[
            pltpu.VMEM((3, win, ny + 16, 2 * nx), jnp.float32),
            pltpu.VMEM((21, ny, zs * nx), jnp.bfloat16),
            pltpu.VMEM((21, ny, zs * nx), jnp.bfloat16),
            pltpu.VMEM((21, ny, zs * nx), jnp.float32),
            pltpu.VMEM((ny, nx), jnp.float32),
            pltpu.VMEM((ny, nx), jnp.float32),
            pltpu.VMEM((ny, ny), jnp.bfloat16),
            pltpu.VMEM((ny, ny), jnp.bfloat16),
        ],
        compiler_params=pltpu.CompilerParams(vmem_limit_bytes=60 * 1024 * 1024),
    )(*blocks, weights, onehot)

    home = lax.all_to_all(back, "pz", split_axis=0, concat_axis=0, tiled=True)
    totals = lax.psum(jnp.sum(home[:, rows:], axis=0), "px")
    stress = home[:, :rows].reshape(n, 6, zs, lp, nx)
    leonard = jnp.transpose(stress, (1, 3, 0, 2, 4)).reshape(6, lp, nz, nx)
    numer, denom = totals[0, :NBIN], totals[4, :NBIN]
    cells = nx * m * nz
    per_bin = numer / jnp.maximum(denom, jnp.float32(cells))
    coefficient = jnp.dot(onehot[:, :NBIN], per_bin, precision=lax.Precision.HIGHEST)
    local_coef = lax.dynamic_slice_in_dim(coefficient, lax.axis_index("pz") * lp, lp, 0)
    viscosity = local_coef[:, None, None] * magnitude
    return (leonard, viscosity, coefficient)


def local(*arrays):
    _, lp, nz, nx = arrays[0].shape
    n, m = lax.axis_size("pz"), lax.axis_size("px")
    groups = nx // nz
    fits = m == 2 and n % 4 == 0 and 8 * n == nx and groups * nz == nx and lp == 16 and groups == 4
    if fits:
        return by_strips(*arrays, n)
    return by_blocks(*arrays)


def solution(mesh):
    return jax.shard_map(
        local,
        mesh=mesh,
        in_specs=(P(None, "pz", None, "px"), P(), P(), P()),
        out_specs=(P(None, "pz", None, "px"), P("pz", None, "px"), P()),
        check_vma=False,
    )
```
